8 devices in a mesh: grp: 1 (over z), dz: 2 (over y), dy: 2 (over x), dx: 2 (over core).
Axes of the slice: x: 2, y: 2, z: 1, core: 2. Of those that a mesh axis runs over, the one named last changes fastest.
Arguments:
- x_in: bfloat16 [8192, 3072], P(('grp', 'dx', 'dz'), 'dy')
- w_gate: bfloat16 [3072, 8192], P('dy', ('dz', 'dx'))
- w_up: bfloat16 [3072, 8192], P('dy', ('dz', 'dx'))
- w_down: bfloat16 [8192, 3072], P('dz', ('dy', 'dx'))
Outputs:
- output: bfloat16 [8192, 3072], P(('grp', 'dx', 'dz'), 'dy')
All inputs are finite; a program needn't handle non-finite values.
Results may differ from the reference program's by a relative error of at most 0.0124721.
Values are sent between devices in bfloat16 or wider.
A program may use at most 1 GiB of HBM per device.

```python
import jax
import jax.numpy as jnp
from jax import lax

N_ROWS = 8192
D_MODEL = 3072
D_FF = 8192
ROW_TILE = 2048


def setup_inputs(seed: int = 0, part: int = 0) -> dict:
    base_key = jax.random.key(seed)
    key_x = jax.random.fold_in(jax.random.fold_in(base_key, 1), part)
    key_gate = jax.random.fold_in(base_key, 2)
    key_up = jax.random.fold_in(base_key, 3)
    key_down = jax.random.fold_in(base_key, 4)
    x_in = jax.random.normal(key_x, (N_ROWS, D_MODEL), jnp.float32).astype(jnp.bfloat16)
    w_gate = (jax.random.normal(key_gate, (D_MODEL, D_FF), jnp.float32) * D_MODEL ** -0.5).astype(jnp.bfloat16)
    w_up = (jax.random.normal(key_up, (D_MODEL, D_FF), jnp.float32) * D_MODEL ** -0.5).astype(jnp.bfloat16)
    w_down = (jax.random.normal(key_down, (D_FF, D_MODEL), jnp.float32) * D_FF ** -0.5).astype(jnp.bfloat16)
    return {"x_in": x_in, "w_gate": w_gate, "w_up": w_up, "w_down": w_down}


def reference(x_in, w_gate, w_up, w_down):
    def row_tile(x_tile):
        gate_val = jnp.dot(x_tile, w_gate, preferred_element_type=jnp.float32).astype(jnp.bfloat16)
        up_val = jnp.dot(x_tile, w_up, preferred_element_type=jnp.float32).astype(jnp.bfloat16)
        hidden = (jax.nn.silu(gate_val.astype(jnp.float32)) * up_val.astype(jnp.float32)).astype(jnp.bfloat16)
        return jnp.dot(hidden, w_down, preferred_element_type=jnp.float32).astype(jnp.bfloat16)
    x_tiles = x_in.reshape(N_ROWS // ROW_TILE, ROW_TILE, D_MODEL)
    return lax.map(row_tile, x_tiles).reshape(N_ROWS, D_MODEL)
```

```python
import jax
import jax.numpy as jnp
from jax import lax
from jax.experimental import pallas as pl
from jax.experimental.pallas import tpu as pltpu
from jax.sharding import PartitionSpec as P

MESH = pl.DeviceIdType.MESH
BF16 = jnp.bfloat16
F32 = jnp.float32


def make_local_mlp(x_shape, w_shape, d_shape):
    rows, dh = x_shape
    fq = w_shape[1]
    fh, dq = d_shape
    ra = rows // 2
    w = 256
    nc = fq // w
    la = 4
    cw = 256
    npr = dq // cw
    nk = 4 * npr
    xc = 2
    xrc = ra // xc
    tm = 512
    own, oth = ra, 0

    def kernel(x, wg, wu, wd,
               z, wdy, wpo, wpx, ddy, dpo, dpx, zr,
               xg, h, wbuf, dbuf, zs, zin, zo,
               xs, xr, wys, wyr, wos, wor, wfs, wfr,
               dys, dyr, dos, dor, dfs, dfr, zss, zsr, zos, zor, zls, lds):
        dz = lax.axis_index("dz")
        dy = lax.axis_index("dy")
        dx = lax.axis_index("dx")
        to_dz = {"dz": 1 - dz}
        to_dy = {"dy": 1 - dy}
        to_dx = {"dx": 1 - dx}

        def rcopy(src, dst, ss, rs, dev):
            return pltpu.make_async_remote_copy(
                src_ref=src, dst_ref=dst, send_sem=ss, recv_sem=rs, device_id=dev, device_id_type=MESH)

        mine = pl.multiple_of(dy * ra, ra)
        theirs = pl.multiple_of((1 - dy) * ra, ra)
        left, right = pl.ds(0, dh), pl.ds(dh, dh)

        def x_dy(i):
            return rcopy(x.at[pl.ds(theirs + i * xrc, xrc)], xg.at[pl.ds(own + i * xrc, xrc), right],
                         xs.at[i], xr.at[i], to_dy)

        def x_fw(i):
            return rcopy(xg.at[pl.ds(own + i * xrc, xrc), right], xg.at[pl.ds(oth + i * xrc, xrc), right],
                         xs.at[xc + i], xr.at[xc + i], to_dz)

        x_dz = rcopy(x.at[pl.ds(mine, ra)], xg.at[pl.ds(oth, ra), left], xs.at[2 * xc], xr.at[2 * xc], to_dz)
        x_lo = pltpu.make_async_copy(x.at[pl.ds(mine, ra)], xg.at[pl.ds(own, ra), left], lds.at[0])

        def cols(j):
            return pl.ds(pl.multiple_of(j * w, w), w)

        def w_dy(j):
            return [rcopy(src.at[:, cols(j)], wdy.at[j, t], wys.at[j, t], wyr.at[j, t], to_dy)
                    for t, src in enumerate((wg, wu))]

        def w_own(j):
            return [rcopy(src.at[:, cols(j)], wpo.at[j, t], wos.at[j, t], wor.at[j, t], to_dx)
                    for t, src in enumerate((wg, wu))]

        def w_fw(j):
            return [rcopy(wdy.at[j, t], wpx.at[j, t], wfs.at[j, t], wfr.at[j, t], to_dx) for t in range(2)]

        def dcols(p):
            return pl.ds(pl.multiple_of(p * cw, cw), cw)

        def d_dy(p):
            return rcopy(wd.at[:, dcols(p)], ddy.at[p], dys.at[p], dyr.at[p], to_dy)

        def d_own(p):
            return rcopy(wd.at[:, dcols(p)], dpo.at[p], dos.at[p], dor.at[p], to_dx)

        def d_fw(p):
            return rcopy(ddy.at[p], dpx.at[p], dfs.at[p], dfr.at[p], to_dx)

        def start(cs):
            for c in cs:
                c.start()

        def wait_all(cs):
            for c in cs:
                c.wait()

        def wait_recv(cs):
            for c in cs:
                c.wait_recv()

        barrier = pltpu.get_barrier_semaphore()
        for dev in (to_dx, to_dy, to_dz):
            pl.semaphore_signal(barrier, inc=1, device_id=dev, device_id_type=MESH)
        pl.semaphore_wait(barrier, 3)

        for i in range(xc):
            x_dy(i).start()
        x_dz.start()
        x_lo.start()

        @pl.loop(0, la)
        def _(j):
            start(w_dy(j))
            start(w_own(j))

        for i in range(xc):
            x_dy(i).wait_recv()
            x_fw(i).start()
        x_lo.wait()
        x_dz.wait_recv()
        for i in range(xc):
            x_fw(i).wait_recv()

        def gate_up(slot, first, last, hcol):
            @pl.loop(first, last)
            def _(r):
                rs = pl.ds(pl.multiple_of(r * tm, tm), tm)
                xt = xg[rs, :]
                g = jnp.dot(xt, wbuf[slot, 0], preferred_element_type=F32).astype(BF16).astype(F32)
                u = jnp.dot(xt, wbuf[slot, 1], preferred_element_type=F32).astype(BF16).astype(F32)
                h[rs, pl.ds(pl.multiple_of(hcol, w), w)] = (g * jax.nn.sigmoid(g) * u).astype(BF16)

        nt = 2 * ra // tm

        @pl.loop(0, nc)
        def _(j):
            @pl.when(j + la < nc)
            def _():
                start(w_dy(j + la))
                start(w_own(j + la))

            @pl.when(jnp.logical_and(j >= la, j < la + npr))
            def _():
                d_dy(j - la).start()
                d_own(j - la).start()

            wait_recv(w_dy(j))
            start(w_fw(j))
            ld0 = [pltpu.make_async_copy(wg.at[:, cols(j)], wbuf.at[0, 0, left], lds.at[0]),
                   pltpu.make_async_copy(wu.at[:, cols(j)], wbuf.at[0, 1, left], lds.at[1]),
                   pltpu.make_async_copy(wdy.at[j, 0], wbuf.at[0, 0, right], lds.at[2]),
                   pltpu.make_async_copy(wdy.at[j, 1], wbuf.at[0, 1, right], lds.at[3])]
            start(ld0)
            wait_all(ld0)
            gate_up(0, 0, nt // 2, dx * fq + j * w)
            wait_recv(w_own(j))
            wait_recv(w_fw(j))
            ld1 = [pltpu.make_async_copy(wpo.at[j, 0], wbuf.at[1, 0, left], lds.at[4]),
                   pltpu.make_async_copy(wpo.at[j, 1], wbuf.at[1, 1, left], lds.at[5]),
                   pltpu.make_async_copy(wpx.at[j, 0], wbuf.at[1, 0, right], lds.at[6]),
                   pltpu.make_async_copy(wpx.at[j, 1], wbuf.at[1, 1, right], lds.at[7])]
            start(ld1)
            gate_up(0, nt // 2, nt, dx * fq + j * w)
            wait_all(ld1)
            gate_up(1, 0, nt, (1 - dx) * fq + j * w)

        def split(k):
            return k // (2 * npr), (k % (2 * npr)) // 2, k % 2

        def load_d(k, slot):
            half, p, q = split(k)
            for hh in range(2):
                for qq in range(2):
                    @pl.when(jnp.logical_and(half == hh, q == qq))
                    def _(hh=hh, qq=qq):
                        src = ((wd.at[:, dcols(p)], dpo.at[p]), (ddy.at[p], dpx.at[p]))[hh][qq]
                        c = pltpu.make_async_copy(src, dbuf.at[slot], lds.at[slot])
                        c.start()
                        c.wait()

        def z_send(k):
            return rcopy(zs.at[k % 3], zr.at[k], zss.at[k], zsr.at[k], to_dz)

        def out_cols(m):
            _, p, q = split(m)
            return pl.ds(pl.multiple_of(((dx + q) % 2) * dq + p * cw, cw), cw)

        def out_local(m):
            return pltpu.make_async_copy(zo.at[m % 2], z.at[pl.ds(mine, ra), out_cols(m)], zls.at[m % 2])

        def out_remote(m):
            i = m - 2 * npr
            return rcopy(zo.at[m % 2], z.at[pl.ds(mine, ra), out_cols(m)], zos.at[i], zor.at[i], to_dy)

        def in_remote(m):
            i = m - 2 * npr
            return rcopy(zo.at[m % 2], z.at[pl.ds(theirs, ra), out_cols(m)], zos.at[i], zor.at[i], to_dy)

        @pl.loop(0, nk + 2)
        def _(k):
            half, p, q = split(k)

            @pl.when(k < nk)
            def _():
                @pl.when(jnp.logical_and(half == 0, q == 1))
                def _():
                    d_own(p).wait_recv()

                @pl.when(jnp.logical_and(half == 1, q == 1))
                def _():
                    d_fw(p).wait_recv()

                load_d(k, 0)

                @pl.when(k >= 3)
                def _():
                    z_send(k - 3).wait_send()

                @pl.loop(0, ra // tm)
                def _(r):
                    rs = pl.ds(pl.multiple_of(r * tm, tm), tm)
                    zs[k % 3, rs] = jnp.dot(h[pl.ds(pl.multiple_of(oth + r * tm, tm), tm), :], dbuf[0],
                                            preferred_element_type=F32)

                z_send(k).start()

            f = k - (2 * npr - 1)

            @pl.when(jnp.logical_and(f >= 0, jnp.logical_and(f < 2 * npr, f % 2 == 0)))
            def _():
                d_dy(f // 2).wait_recv()
                d_fw(f // 2).start()

            @pl.when(k >= 2)
            def _():
                m = k - 2
                load_d(m, 1)
                z_send(m).wait_recv()
                c = pltpu.make_async_copy(zr.at[m], zin, lds.at[2])
                c.start()

                @pl.when(jnp.logical_and(m >= 2, m < 2 * npr + 2))
                def _():
                    out_local(m - 2).wait()

                @pl.when(m >= 2 * npr + 2)
                def _():
                    out_remote(m - 2).wait_send()

                c.wait()

                @pl.loop(0, ra // tm)
                def _(r):
                    rs = pl.ds(pl.multiple_of(r * tm, tm), tm)
                    acc = jnp.dot(h[pl.ds(pl.multiple_of(own + r * tm, tm), tm), :], dbuf[1],
                                  preferred_element_type=F32)
                    zo[m % 2, rs] = (acc + zin[rs]).astype(BF16)

                @pl.when(m < 2 * npr)
                def _():
                    out_local(m).start()

                @pl.when(m >= 2 * npr)
                def _():
                    out_remote(m).start()

        for m in (nk - 2, nk - 1):
            out_remote(m).wait_send()
        for m in range(2 * npr, nk):
            in_remote(m).wait_recv()
        for k in range(nk - 3, nk):
            z_send(k).wait_send()
        for i in range(xc):
            x_dy(i).wait_send()
            x_fw(i).wait_send()
        x_dz.wait_send()

        @pl.loop(0, nc)
        def _(j):
            for c in w_dy(j) + w_own(j) + w_fw(j):
                c.wait_send()

        @pl.loop(0, npr)
        def _(p):
            d_dy(p).wait_send()
            d_own(p).wait_send()
            d_fw(p).wait_send()

    def sd(shape, dtype=BF16):
        return jax.ShapeDtypeStruct(shape, dtype)

    wl = sd((nc, 2, dh, w))
    dl = sd((npr, fh, cw))
    outs = (sd((rows, dh)), wl, wl, wl, dl, dl, dl, sd((nk, ra, cw), F32))
    dma = pltpu.SemaphoreType.DMA
    return pl.pallas_call(
        kernel,
        out_shape=outs,
        in_specs=[pl.BlockSpec(memory_space=pl.ANY)] * 4,
        out_specs=[pl.BlockSpec(memory_space=pl.ANY)] * len(outs),
        scratch_shapes=[
            pltpu.VMEM((rows, 2 * dh), BF16),
            pltpu.VMEM((rows, fh), BF16),
            pltpu.VMEM((2, 2, 2 * dh, w), BF16),
            pltpu.VMEM((2, fh, cw), BF16),
            pltpu.VMEM((3, ra, cw), F32),
            pltpu.VMEM((ra, cw), F32),
            pltpu.VMEM((2, ra, cw), BF16),
            dma((2 * xc + 1,)), dma((2 * xc + 1,)),
            dma((nc, 2)), dma((nc, 2)), dma((nc, 2)), dma((nc, 2)), dma((nc, 2)), dma((nc, 2)),
            dma((npr,)), dma((npr,)), dma((npr,)), dma((npr,)), dma((npr,)), dma((npr,)),
            dma((nk,)), dma((nk,)), dma((2 * npr,)), dma((2 * npr,)), dma((2,)), dma((8,)),
        ],
        compiler_params=pltpu.CompilerParams(
            collective_id=0, has_side_effects=True, vmem_limit_bytes=62 * 1024 * 1024),
    )


def solution(mesh):
    x_spec = P(("grp", "dx", "dz"), "dy")
    w_in_spec = P("dy", ("dz", "dx"))
    w_out_spec = P("dz", ("dy", "dx"))

    def local_mlp(x_blk, wg_blk, wu_blk, wd_blk):
        return make_local_mlp(x_blk.shape, wg_blk.shape, wd_blk.shape)(x_blk, wg_blk, wu_blk, wd_blk)[0]

    return jax.shard_map(local_mlp, mesh=mesh, in_specs=(x_spec, w_in_spec, w_in_spec, w_out_spec), out_specs=x_spec, check_vma=False)
```

```python
import jax
import jax.numpy as jnp
from jax import lax
from jax.experimental import pallas as pl
from jax.experimental.pallas import tpu as pltpu
from jax.sharding import PartitionSpec as P

MESH = pl.DeviceIdType.MESH
BF16 = jnp.bfloat16
F32 = jnp.float32


def make_local_mlp(x_shape, w_shape, d_shape):
    rows, dh = x_shape
    fq = w_shape[1]
    fh, dq = d_shape
    ra = rows // 2
    w = 256
    nc = fq // w
    la = 4
    cw = 256
    npr = dq // cw
    tm = 512
    nz = ra // tm
    ne = tm
    ve = npr - 1
    xc = 2
    xrc = ra // xc
    nl = 2 * ve
    nk = nl + nz * (4 * npr - 2 * ve)
    no = nz * 2 * npr
    lag = 3
    own, oth = ra, 0

    def kernel(x, wg, wu, wd,
               z, wdy, wpo, wpx, ddy, dpo, dpx, d2o, d2p, zr,
               xg, h, h2, wbuf, dbuf, zs, zin, zacc, zo,
               xs, xr, wys, wyr, wos, wor, wfs, wfr, hs, hr,
               dys, dyr, dos, dor, dfs, dfr, d2s, d2r, d2t, d2u,
               zss, zsr, zos, zor, zls, lds):
        dz = lax.axis_index("dz")
        dy = lax.axis_index("dy")
        dx = lax.axis_index("dx")
        to_dz = {"dz": 1 - dz}
        to_dy = {"dy": 1 - dy}
        to_dx = {"dx": 1 - dx}

        def rcopy(src, dst, ss, rs, dev):
            return pltpu.make_async_remote_copy(
                src_ref=src, dst_ref=dst, send_sem=ss, recv_sem=rs, device_id=dev, device_id_type=MESH)

        mine = pl.multiple_of(dy * ra, ra)
        theirs = pl.multiple_of((1 - dy) * ra, ra)
        left, right = pl.ds(0, dh), pl.ds(dh, dh)

        def x_dy(i):
            return rcopy(x.at[pl.ds(theirs + i * xrc, xrc)], xg.at[pl.ds(own + i * xrc, xrc), right],
                         xs.at[i], xr.at[i], to_dy)

        def x_fw(i):
            return rcopy(xg.at[pl.ds(own + i * xrc, xrc), right], xg.at[pl.ds(oth + i * xrc, xrc), right],
                         xs.at[xc + i], xr.at[xc + i], to_dz)

        x_dz = rcopy(x.at[pl.ds(mine, ra)], xg.at[pl.ds(oth, ra), left], xs.at[2 * xc], xr.at[2 * xc], to_dz)
        x_lo = pltpu.make_async_copy(x.at[pl.ds(mine, ra)], xg.at[pl.ds(own, ra), left], lds.at[0])

        def cols(j):
            return pl.ds(pl.multiple_of(j * w, w), w)

        def w_dy(j):
            return [rcopy(src.at[:, cols(j)], wdy.at[j, t], wys.at[j, t], wyr.at[j, t], to_dy)
                    for t, src in enumerate((wg, wu))]

        def w_own(j):
            return [rcopy(src.at[:, cols(j)], wpo.at[j, t], wos.at[j, t], wor.at[j, t], to_dx)
                    for t, src in enumerate((wg, wu))]

        def w_fw(j):
            return [rcopy(wdy.at[j, t], wpx.at[j, t], wfs.at[j, t], wfr.at[j, t], to_dx) for t in range(2)]

        def dcols(p):
            return pl.ds(pl.multiple_of(p * cw, cw), cw)

        def d_dy(p):
            return rcopy(wd.at[:, dcols(p)], ddy.at[p], dys.at[p], dyr.at[p], to_dy)

        def d_own(p):
            return rcopy(wd.at[:, dcols(p)], dpo.at[p], dos.at[p], dor.at[p], to_dx)

        def d_fw(p):
            return rcopy(ddy.at[p], dpx.at[p], dfs.at[p], dfr.at[p], to_dx)

        def d2_dz(p):
            return rcopy(wd.at[:, dcols(p)], d2o.at[p], d2s.at[p], d2r.at[p], to_dz)

        def d2_fw(p):
            return rcopy(d2o.at[p], d2p.at[p], d2t.at[p], d2u.at[p], to_dx)

        def hcols(j, t):
            return pl.ds(pl.multiple_of(((dx + t) % 2) * fq + j * w, w), w)

        def h_dz(j, t):
            return rcopy(h.at[pl.ds(oth, ne), hcols(j, t)], h2.at[:, hcols(j, t)], hs.at[j, t], hr.at[j, t], to_dz)

        def start(cs):
            for c in cs:
                c.start()

        def wait_all(cs):
            for c in cs:
                c.wait()

        def wait_recv(cs):
            for c in cs:
                c.wait_recv()

        barrier = pltpu.get_barrier_semaphore()
        for dev in (to_dx, to_dy, to_dz):
            pl.semaphore_signal(barrier, inc=1, device_id=dev, device_id_type=MESH)
        pl.semaphore_wait(barrier, 3)

        for i in range(xc):
            x_dy(i).start()
        x_dz.start()
        x_lo.start()

        @pl.loop(0, la)
        def _(j):
            start(w_dy(j))
            start(w_own(j))

        for i in range(xc):
            x_dy(i).wait_recv()
            x_fw(i).start()
        for p in range(ve):
            d2_dz(p).start()
        x_lo.wait()
        x_dz.wait_recv()
        for i in range(xc):
            x_fw(i).wait_recv()

        def gate_up(slot, row, hc):
            rs = pl.ds(pl.multiple_of(row, tm), tm)
            xt = xg[rs, :]
            g = jnp.dot(xt, wbuf[slot, 0], preferred_element_type=F32).astype(BF16).astype(F32)
            u = jnp.dot(xt, wbuf[slot, 1], preferred_element_type=F32).astype(BF16).astype(F32)
            h[rs, hc] = (g * jax.nn.sigmoid(g) * u).astype(BF16)

        def own_rows(j):
            @pl.loop(0, 2 * nz)
            def _(i):
                t = i // nz
                gate_up(t, own + (i % nz) * tm, hcols(j, t))

        @pl.loop(0, nc)
        def _(j):
            @pl.when(j + la < nc)
            def _():
                start(w_dy(j + la))
                start(w_own(j + la))

            @pl.when(jnp.logical_and(j >= la, j < la + npr))
            def _():
                d_dy(j - la).start()
                d_own(j - la).start()

            @pl.when(jnp.logical_and(j >= la + 1, j < la + 1 + ve))
            def _():
                d2_dz(j - la - 1).wait_recv()
                d2_fw(j - la - 1).start()

            wait_recv(w_dy(j))
            start(w_fw(j))
            ld0 = [pltpu.make_async_copy(wg.at[:, cols(j)], wbuf.at[0, 0, left], lds.at[0]),
                   pltpu.make_async_copy(wu.at[:, cols(j)], wbuf.at[0, 1, left], lds.at[1]),
                   pltpu.make_async_copy(wdy.at[j, 0], wbuf.at[0, 0, right], lds.at[2]),
                   pltpu.make_async_copy(wdy.at[j, 1], wbuf.at[0, 1, right], lds.at[3])]
            start(ld0)
            wait_all(ld0)
            ld1 = [pltpu.make_async_copy(wpo.at[j, 0], wbuf.at[1, 0, left], lds.at[4]),
                   pltpu.make_async_copy(wpo.at[j, 1], wbuf.at[1, 1, left], lds.at[5]),
                   pltpu.make_async_copy(wpx.at[j, 0], wbuf.at[1, 0, right], lds.at[6]),
                   pltpu.make_async_copy(wpx.at[j, 1], wbuf.at[1, 1, right], lds.at[7])]

            @pl.loop(0, 2 * nz)
            def _(i):
                t = i // nz

                @pl.when(i == 1)
                def _():
                    wait_recv(w_own(j))
                    wait_recv(w_fw(j))
                    start(ld1)

                @pl.when(i == nz)
                def _():
                    wait_all(ld1)

                gate_up(t, oth + (i % nz) * tm, hcols(j, t))

                @pl.when(i >= nz)
                def _():
                    h_dz(j, i - nz).start()

            @pl.when(j < nc - 1)
            def _():
                own_rows(j)

        def split(k):
            late = (k + nk - nl) // nk
            s = (k - nl) // nz + nk
            first = s - nk
            lastc = 2 * npr + 1
            other = (first + lastc - 1) // lastc - first // lastc
            half = late * other
            p = (1 - late) * (k // 2) + late * (other * ((first + 2 * npr - 1) // 2 - npr) + (1 - other) * (npr - 1))
            q = (1 - late) * (k % 2) + late * (other * ((first + 1) % 2) + (1 - other) * (first // lastc))
            r = (1 - late) * (nz - 1) + late * ((k + nl) % nz)
            return half, p, q, r

        def chunk_src(half, p, q):
            return ((wd.at[:, dcols(p)], dpo.at[p]), (ddy.at[p], dpx.at[p]))[half][q]

        def load_d(k, slot):
            half, p, q, r = split(k)
            for hh in range(2):
                for qq in range(2):
                    @pl.when(jnp.logical_and(jnp.logical_or(k < nl, r == 0), jnp.logical_and(half == hh, q == qq)))
                    def _(hh=hh, qq=qq):
                        c = pltpu.make_async_copy(chunk_src(hh, p, qq), dbuf.at[slot], lds.at[slot])
                        c.start()
                        c.wait()

        def z_send(k):
            return rcopy(zs.at[k % (lag + 1)], zr.at[k], zss.at[k], zsr.at[k], to_dz)

        def out_cols(p, q):
            return pl.ds(pl.multiple_of(((dx + q) % 2) * dq + p * cw, cw), cw)

        def out_at(m, base):
            half, p, q, r = split(m)
            return z.at[pl.ds(pl.multiple_of(base + r * tm, tm), tm), out_cols(p, q)]

        def is_other(m):
            return split(m)[0] == 1

        def out_local(m):
            return pltpu.make_async_copy(zo.at[m % 2], out_at(m, mine), zls.at[m % 2])

        def out_remote(m):
            i = m - (nl + nz)
            return rcopy(zo.at[m % 2], out_at(m, mine), zos.at[i], zor.at[i], to_dy)

        def in_remote(m):
            i = m - (nl + nz)
            return rcopy(zo.at[m % 2], out_at(m, theirs), zos.at[i], zor.at[i], to_dy)

        def free_out(m):
            @pl.when(is_other(m))
            def _():
                out_remote(m).wait_send()

            @pl.when(jnp.logical_not(is_other(m)))
            def _():
                out_local(m).wait()

        def send_piece(k):
            half, p, q, r = split(k)

            @pl.when(jnp.logical_and(q == 1, jnp.logical_or(k < nl, r == 0)))
            def _():
                @pl.when(half == 0)
                def _():
                    d_own(p).wait_recv()

                @pl.when(half == 1)
                def _():
                    d_fw(p).wait_recv()

            load_d(k, 0)

            @pl.when(k > lag)
            def _():
                z_send(k - lag - 1).wait_send()

            zs[k % (lag + 1)] = jnp.dot(h[pl.ds(pl.multiple_of(oth + r * tm, tm), tm), :], dbuf[0],
                                        preferred_element_type=F32)
            z_send(k).start()

        def e_out(e):
            return pltpu.make_async_copy(zo.at[2], z.at[pl.ds(mine, ne), out_cols(e // 2, e % 2)], zls.at[2])

        def e_piece(e):
            p = e // 2
            for qq in range(2):
                @pl.when(e % 2 == qq)
                def _(qq=qq):
                    c = [pltpu.make_async_copy(chunk_src(0, p, qq), dbuf.at[2], lds.at[2]),
                         pltpu.make_async_copy((d2o, d2p)[qq].at[p], dbuf.at[3], lds.at[3])]
                    start(c)
                    wait_all(c)

            acc = jnp.dot(h[pl.ds(own, ne), :], dbuf[2], preferred_element_type=F32)
            acc = acc + jnp.dot(h2[...], dbuf[3], preferred_element_type=F32)

            @pl.when(e >= 1)
            def _():
                e_out(e - 1).wait()

            zo[2] = acc.astype(BF16)
            e_out(e).start()

        e0 = 5

        @pl.loop(0, nk + lag)
        def _(k):
            @pl.when(k < nk)
            def _():
                send_piece(k)

            @pl.when(k == lag - 1)
            def _():
                own_rows(nc - 1)

            f = k - (nl + nz - 1)

            @pl.when(jnp.logical_and(f >= 0, jnp.logical_and(f < 2 * nz * npr, f % (2 * nz) == 0)))
            def _():
                d_dy(f // (2 * nz)).wait_recv()
                d_fw(f // (2 * nz)).start()

            @pl.when(k == e0 - 1)
            def _():
                for p in range(ve):
                    d2_fw(p).wait_recv()

                @pl.loop(0, nc)
                def _(j):
                    for t in range(2):
                        h_dz(j, t).wait_recv()

            @pl.when(jnp.logical_and(k >= e0, jnp.logical_and(k < e0 + 4 * ve, (k - e0) % 2 == 0)))
            def _():
                e_piece((k - e0) // 2)

            @pl.when(k >= lag)
            def _():
                m = k - lag
                half, p, q, r = split(m)
                load_d(m, 1)
                zacc[...] = jnp.dot(h[pl.ds(pl.multiple_of(own + r * tm, tm), tm), :], dbuf[1],
                                    preferred_element_type=F32)

                @pl.when(m >= 2)
                def _():
                    free_out(m - 2)

                z_send(m).wait_recv()
                c = pltpu.make_async_copy(zr.at[m], zin, lds.at[4])
                c.start()
                c.wait()
                zo[m % 2] = (zacc[...] + zin[...]).astype(BF16)

                @pl.when(half == 0)
                def _():
                    out_local(m).start()

                @pl.when(half == 1)
                def _():
                    out_remote(m).start()

        for m in (nk - 2, nk - 1):
            out_local(m).wait()
        e_out(2 * ve - 1).wait()
        for k in range(nk - lag - 1, nk):
            z_send(k).wait_send()
        for i in range(xc):
            x_dy(i).wait_send()
            x_fw(i).wait_send()
        x_dz.wait_send()

        @pl.loop(0, nc)
        def _(j):
            for c in w_dy(j) + w_own(j) + w_fw(j) + [h_dz(j, 0), h_dz(j, 1)]:
                c.wait_send()

        @pl.loop(0, npr)
        def _(p):
            d_dy(p).wait_send()
            d_own(p).wait_send()
            d_fw(p).wait_send()

        @pl.loop(0, ve)
        def _(p):
            d2_dz(p).wait_send()
            d2_fw(p).wait_send()

        @pl.loop(nl + nz, nl + nz + no)
        def _(m):
            in_remote(m).wait_recv()

    def sd(shape, dtype=BF16):
        return jax.ShapeDtypeStruct(shape, dtype)

    wl = sd((nc, 2, dh, w))
    dl = sd((npr, fh, cw))
    el = sd((ve, fh, cw))
    outs = (sd((rows, dh)), wl, wl, wl, dl, dl, dl, el, el, sd((nk, tm, cw), F32))
    dma = pltpu.SemaphoreType.DMA
    return pl.pallas_call(
        kernel,
        out_shape=outs,
        in_specs=[pl.BlockSpec(memory_space=pl.ANY)] * 4,
        out_specs=[pl.BlockSpec(memory_space=pl.ANY)] * len(outs),
        scratch_shapes=[
            pltpu.VMEM((rows, 2 * dh), BF16),
            pltpu.VMEM((rows, fh), BF16),
            pltpu.VMEM((ne, fh), BF16),
            pltpu.VMEM((2, 2, 2 * dh, w), BF16),
            pltpu.VMEM((4, fh, cw), BF16),
            pltpu.VMEM((lag + 1, tm, cw), F32),
            pltpu.VMEM((tm, cw), F32),
            pltpu.VMEM((tm, cw), F32),
            pltpu.VMEM((3, tm, cw), BF16),
            dma((2 * xc + 1,)), dma((2 * xc + 1,)),
            dma((nc, 2)), dma((nc, 2)), dma((nc, 2)), dma((nc, 2)), dma((nc, 2)), dma((nc, 2)), dma((nc, 2)), dma((nc, 2)),
            dma((npr,)), dma((npr,)), dma((npr,)), dma((npr,)), dma((npr,)), dma((npr,)),
            dma((ve,)), dma((ve,)), dma((ve,)), dma((ve,)),
            dma((nk,)), dma((nk,)), dma((no,)), dma((no,)), dma((3,)), dma((8,)),
        ],
        compiler_params=pltpu.CompilerParams(
            collective_id=0, has_side_effects=True, vmem_limit_bytes=62 * 1024 * 1024),
    )


def solution(mesh):
    x_spec = P(("grp", "dx", "dz"), "dy")
    w_in_spec = P("dy", ("dz", "dx"))
    w_out_spec = P("dz", ("dy", "dx"))

    def local_mlp(x_blk, wg_blk, wu_blk, wd_blk):
        return make_local_mlp(x_blk.shape, wg_blk.shape, wd_blk.shape)(x_blk, wg_blk, wu_blk, wd_blk)[0]

    return jax.shard_map(local_mlp, mesh=mesh, in_specs=(x_spec, w_in_spec, w_in_spec, w_out_spec), out_specs=x_spec, check_vma=False)
```

```python
import jax
import jax.numpy as jnp
from jax import lax
from jax.experimental import pallas as pl
from jax.experimental.pallas import tpu as pltpu
from jax.sharding import PartitionSpec as P

MESH = pl.DeviceIdType.MESH
BF16 = jnp.bfloat16
F32 = jnp.float32


def make_local_mlp(x_shape, w_shape, d_shape):
    rows, dh = x_shape
    fq = w_shape[1]
    fh, dq = d_shape
    ra = rows // 2
    w = 128
    nc = fq // w
    la = 8
    cw = 256
    npr = dq // cw
    tm = 512
    nz = ra // tm
    ne = tm
    nl = 2 * npr - 1
    nk = nl + nz * (4 * npr - nl)
    no = nz * 2 * npr
    lag = 3
    xc = 2
    xrc = ra // xc
    own, oth = ra, 0

    def kernel(x, wg, wu, wd,
               z, wdy, wpo, wpx, ddy, dpo, dpx, d2o, d2p, zr,
               xg, h, h2, wbuf, dbuf, zs, zin, zacc, zo,
               xs, xr, wys, wyr, wfs, wfr, hs, hr, bs, br,
               dys, dyr, dfs, dfr, d2s, d2r, d2t, d2u,
               zss, zsr, zos, zor, zls, lds):
        dz = lax.axis_index("dz")
        dy = lax.axis_index("dy")
        dx = lax.axis_index("dx")
        to_dz = {"dz": 1 - dz}
        to_dy = {"dy": 1 - dy}
        to_dx = {"dx": 1 - dx}

        def rcopy(src, dst, ss, rs, dev):
            return pltpu.make_async_remote_copy(
                src_ref=src, dst_ref=dst, send_sem=ss, recv_sem=rs, device_id=dev, device_id_type=MESH)

        mine = pl.multiple_of(dy * ra, ra)
        theirs = pl.multiple_of((1 - dy) * ra, ra)
        left, right = pl.ds(0, dh), pl.ds(dh, dh)

        def x_dy(i):
            return rcopy(x.at[pl.ds(theirs + i * xrc, xrc)], xg.at[pl.ds(own + i * xrc, xrc), right],
                         xs.at[i], xr.at[i], to_dy)

        def x_fw(i):
            return rcopy(xg.at[pl.ds(own + i * xrc, xrc), right], xg.at[pl.ds(oth + i * xrc, xrc), right],
                         xs.at[xc + i], xr.at[xc + i], to_dz)

        x_dz = rcopy(x.at[pl.ds(mine, ra)], xg.at[pl.ds(oth, ra), left], xs.at[2 * xc], xr.at[2 * xc], to_dz)
        x_lo = pltpu.make_async_copy(x.at[pl.ds(mine, ra)], xg.at[pl.ds(own, ra), left], lds.at[8])

        def cols(j):
            return pl.ds(pl.multiple_of(j * w, w), w)

        def w_dy(j):
            return [rcopy(src.at[:, cols(j)], wdy.at[j, t], wys.at[j, t], wyr.at[j, t], to_dy)
                    for t, src in enumerate((wg, wu))]

        def w_fw(j):
            return [rcopy(wdy.at[j, t], wpx.at[j, t], wfs.at[j, t], wfr.at[j, t], to_dx) for t in range(2)]

        def dcols(p):
            return pl.ds(pl.multiple_of(p * cw, cw), cw)

        def d_dy(p):
            return rcopy(wd.at[:, dcols(p)], ddy.at[p], dys.at[p], dyr.at[p], to_dy)

        def d_fw(p):
            return rcopy(ddy.at[p], dpx.at[p], dfs.at[p], dfr.at[p], to_dx)

        bulk = [rcopy(src, dst, bs.at[i], br.at[i], to_dx)
                for i, (src, dst) in enumerate(((wg, wpo.at[0]), (wu, wpo.at[1]), (wd, dpo)))]

        def d2_dz(p):
            return rcopy(wd.at[:, dcols(p)], d2o.at[p], d2s.at[p], d2r.at[p], to_dz)

        def d2_fw(p):
            return rcopy(d2o.at[p], d2p.at[p], d2t.at[p], d2u.at[p], to_dx)

        def hcols(j, t):
            return pl.ds(pl.multiple_of(((dx + t) % 2) * fq + j * w, w), w)

        def h_dz(j, t):
            return rcopy(h.at[pl.ds(oth, ne), hcols(j, t)], h2.at[:, hcols(j, t)], hs.at[j, t], hr.at[j, t], to_dz)

        def start(cs):
            for c in cs:
                c.start()

        def wait_all(cs):
            for c in cs:
                c.wait()

        def wait_recv(cs):
            for c in cs:
                c.wait_recv()

        barrier = pltpu.get_barrier_semaphore()
        for dev in (to_dx, to_dy, to_dz):
            pl.semaphore_signal(barrier, inc=1, device_id=dev, device_id_type=MESH)
        pl.semaphore_wait(barrier, 3)

        for i in range(xc):
            x_dy(i).start()
        x_dz.start()
        x_lo.start()

        @pl.loop(0, la)
        def _(j):
            start(w_dy(j))

        for i in range(xc):
            x_dy(i).wait_recv()
            x_fw(i).start()
        for p in range(npr - 1):
            d2_dz(p).start()

        @pl.when(dx == 0)
        def _():
            d2_dz(npr - 1).start()

        start(bulk)
        x_lo.wait()
        first_d = pltpu.make_async_copy(wd.at[:, dcols(0)], dbuf.at[0], lds.at[8])
        first_d.start()
        x_dz.wait_recv()
        for i in range(xc):
            x_fw(i).wait_recv()
        wait_recv(bulk)

        def gate_up(row, j):
            rs = pl.ds(pl.multiple_of(row, tm), tm)
            xt = xg[rs, :]
            g = jnp.dot(xt, wbuf[0], preferred_element_type=F32).astype(BF16).astype(F32)
            u = jnp.dot(xt, wbuf[1], preferred_element_type=F32).astype(BF16).astype(F32)
            val = (g * jax.nn.sigmoid(g) * u).astype(BF16)
            for t in range(2):
                h[rs, hcols(j, t)] = val[:, t * w:(t + 1) * w]

        def rest(j):
            @pl.loop(0, nz + 1)
            def _(i):
                gate_up((i + (i + nz) // (nz + 1)) * tm, j)

                @pl.when(i == 1)
                def _():
                    h_dz(j, 0).start()
                    h_dz(j, 1).start()

        @pl.loop(0, nc)
        def _(j):
            @pl.when(j + la < nc)
            def _():
                start(w_dy(j + la))

            @pl.when(jnp.logical_and(j >= la, j < la + npr))
            def _():
                d_dy(j - la).start()

            @pl.when(jnp.logical_and(j >= nc - npr - 1, j < nc - 2))
            def _():
                p = j - (nc - npr - 1)
                d2_dz(p).wait_recv()
                d2_fw(p).start()

            @pl.when(jnp.logical_and(dx == 0, j == nc - 2))
            def _():
                d2_dz(npr - 1).wait_recv()
                d2_fw(npr - 1).start()

            wait_recv(w_dy(j))
            start(w_fw(j))
            la_, lb_ = pl.ds(0, w), pl.ds(w, w)
            ld0 = [pltpu.make_async_copy(wg.at[:, cols(j)], wbuf.at[0, left, la_], lds.at[0]),
                   pltpu.make_async_copy(wu.at[:, cols(j)], wbuf.at[1, left, la_], lds.at[1]),
                   pltpu.make_async_copy(wpo.at[0, :, cols(j)], wbuf.at[0, left, lb_], lds.at[2]),
                   pltpu.make_async_copy(wpo.at[1, :, cols(j)], wbuf.at[1, left, lb_], lds.at[3]),
                   pltpu.make_async_copy(wdy.at[j, 0], wbuf.at[0, right, la_], lds.at[4]),
                   pltpu.make_async_copy(wdy.at[j, 1], wbuf.at[1, right, la_], lds.at[5])]
            ld1 = [pltpu.make_async_copy(wpx.at[j, 0], wbuf.at[0, right, lb_], lds.at[6]),
                   pltpu.make_async_copy(wpx.at[j, 1], wbuf.at[1, right, lb_], lds.at[7])]
            start(ld0)
            wait_recv(w_fw(j))
            start(ld1)
            wait_all(ld0 + ld1)
            gate_up(oth + (nz - 1) * tm, j)

            @pl.when(j < nc - 1)
            def _():
                rest(j)

        def split(k):
            late = (k + nk - nl) // nk
            s = (k - nl) // nz
            last = s // (2 * npr)
            odd = k // (nl - 1)
            half = late * (1 - last)
            p = (1 - late) * (k // 2) + late * ((1 - last) * (s // 2) + last * (npr - 1))
            q = (1 - late) * ((1 - odd) * (k % 2) + odd * dx) + late * ((1 - last) * (s % 2) + last * (1 - dx))
            r = (1 - late) * (nz - 1) + late * ((k - nl) % nz)
            return half, p, q, r

        def chunk_src(half, p, q):
            if half == 0:
                return (wd, dpo)[q].at[:, dcols(p)]
            return (ddy, dpx)[q].at[p]

        def load_d(k, slot, ok):
            half, p, q, r = split(k)
            ok = jnp.logical_and(ok, jnp.logical_or(k < nl, r == 0))
            for hh in range(2):
                for qq in range(2):
                    @pl.when(jnp.logical_and(ok, jnp.logical_and(half == hh, q == qq)))
                    def _(hh=hh, qq=qq):
                        c = pltpu.make_async_copy(chunk_src(hh, p, qq), dbuf.at[slot], lds.at[slot])
                        c.start()
                        c.wait()

        def z_send(k):
            return rcopy(zs.at[k % (lag + 1)], zr.at[k], zss.at[k], zsr.at[k], to_dz)

        def out_cols(p, q):
            return pl.ds(pl.multiple_of(((dx + q) % 2) * dq + p * cw, cw), cw)

        def out_at(m, base):
            half, p, q, r = split(m)
            return z.at[pl.ds(pl.multiple_of(base + r * tm, tm), tm), out_cols(p, q)]

        def is_other(m):
            return split(m)[0] == 1

        def out_local(m):
            return pltpu.make_async_copy(zo.at[m % 2], out_at(m, mine), zls.at[m % 2])

        def out_remote(m):
            i = m - nl
            return rcopy(zo.at[m % 2], out_at(m, mine), zos.at[i], zor.at[i], to_dy)

        def in_remote(m):
            i = m - nl
            return rcopy(zo.at[m % 2], out_at(m, theirs), zos.at[i], zor.at[i], to_dy)

        def free_out(m):
            @pl.when(is_other(m))
            def _():
                out_remote(m).wait_send()

            @pl.when(jnp.logical_not(is_other(m)))
            def _():
                out_local(m).wait()

        def send_piece(k):
            half, p, q, r = split(k)

            @pl.when(jnp.logical_and(jnp.logical_and(half == 1, q == 1), r == 0))
            def _():
                d_fw(p).wait_recv()

            @pl.when(k == 0)
            def _():
                first_d.wait()

            load_d(k, 0, k > 0)

            @pl.when(k > lag)
            def _():
                z_send(k - lag - 1).wait_send()

            zs[k % (lag + 1)] = jnp.dot(h[pl.ds(pl.multiple_of(oth + r * tm, tm), tm), :], dbuf[0],
                                        preferred_element_type=F32)
            z_send(k).start()

        def e_out(e):
            _, p, q, _ = split(e)
            return pltpu.make_async_copy(zo.at[2], z.at[pl.ds(mine, ne), out_cols(p, q)], zls.at[2])

        def e_piece(e):
            _, p, q, _ = split(e)
            for qq in range(2):
                @pl.when(q == qq)
                def _(qq=qq):
                    c = [pltpu.make_async_copy(chunk_src(0, p, qq), dbuf.at[2], lds.at[2]),
                         pltpu.make_async_copy((d2o, d2p)[qq].at[p], dbuf.at[3], lds.at[3])]
                    start(c)
                    wait_all(c)

            acc = jnp.dot(h[pl.ds(own, ne), :], dbuf[2], preferred_element_type=F32)
            acc = acc + jnp.dot(h2[...], dbuf[3], preferred_element_type=F32)

            @pl.when(e >= 1)
            def _():
                e_out(e - 1).wait()

            zo[2] = acc.astype(BF16)
            e_out(e).start()

        e0 = 7

        @pl.loop(0, nk + lag)
        def _(k):
            @pl.when(k < nk)
            def _():
                send_piece(k)

            @pl.when(k == lag - 1)
            def _():
                rest(nc - 1)

            f = k - (nl - 1)

            @pl.when(jnp.logical_and(f >= 0, jnp.logical_and(f < 2 * nz * npr, f % (2 * nz) == 0)))
            def _():
                d_dy(f // (2 * nz)).wait_recv()
                d_fw(f // (2 * nz)).start()

            @pl.when(k == e0 - 1)
            def _():
                for p in range(npr - 1):
                    d2_fw(p).wait_recv()

                @pl.when(dx == 1)
                def _():
                    d2_fw(npr - 1).wait_recv()

                @pl.loop(0, nc)
                def _(j):
                    for t in range(2):
                        h_dz(j, t).wait_recv()

            @pl.when(jnp.logical_and(k >= e0, jnp.logical_and(k < e0 + 2 * nl, (k - e0) % 2 == 0)))
            def _():
                e_piece((k - e0) // 2)

            @pl.when(k >= lag)
            def _():
                m = k - lag
                half, p, q, r = split(m)
                load_d(m, 1, k >= lag)
                zacc[...] = jnp.dot(h[pl.ds(pl.multiple_of(own + r * tm, tm), tm), :], dbuf[1],
                                    preferred_element_type=F32)

                @pl.when(m >= 2)
                def _():
                    free_out(m - 2)

                z_send(m).wait_recv()
                c = pltpu.make_async_copy(zr.at[m], zin, lds.at[4])
                c.start()
                c.wait()
                zo[m % 2] = (zacc[...] + zin[...]).astype(BF16)

                @pl.when(half == 0)
                def _():
                    out_local(m).start()

                @pl.when(half == 1)
                def _():
                    out_remote(m).start()

        for m in (nk - 2, nk - 1):
            out_local(m).wait()
        e_out(nl - 1).wait()
        for k in range(nk - lag - 1, nk):
            z_send(k).wait_send()
        for i in range(xc):
            x_dy(i).wait_send()
            x_fw(i).wait_send()
        x_dz.wait_send()

        @pl.loop(0, nc)
        def _(j):
            for c in w_dy(j) + w_fw(j) + [h_dz(j, 0), h_dz(j, 1)]:
                c.wait_send()

        @pl.loop(0, npr)
        def _(p):
            d_dy(p).wait_send()
            d_fw(p).wait_send()

        for c in bulk:
            c.wait_send()
        for p in range(npr - 1):
            d2_dz(p).wait_send()
            d2_fw(p).wait_send()

        @pl.when(dx == 0)
        def _():
            d2_dz(npr - 1).wait_send()
            d2_fw(npr - 1).wait_send()

        @pl.loop(nl, nl + no)
        def _(m):
            in_remote(m).wait_recv()

    def sd(shape, dtype=BF16):
        return jax.ShapeDtypeStruct(shape, dtype)

    wl, dl = sd((nc, 2, dh, w)), sd((npr, fh, cw))
    outs = (sd((rows, dh)), wl, sd((2, dh, fq)), wl, dl, sd((fh, dq)), dl, dl, dl, sd((nk, tm, cw), F32))
    dma = pltpu.SemaphoreType.DMA
    return pl.pallas_call(
        kernel,
        out_shape=outs,
        in_specs=[pl.BlockSpec(memory_space=pl.ANY)] * 4,
        out_specs=[pl.BlockSpec(memory_space=pl.ANY)] * len(outs),
        scratch_shapes=[
            pltpu.VMEM((rows, 2 * dh), BF16),
            pltpu.VMEM((rows, fh), BF16),
            pltpu.VMEM((ne, fh), BF16),
            pltpu.VMEM((2, 2 * dh, 2 * w), BF16),
            pltpu.VMEM((4, fh, cw), BF16),
            pltpu.VMEM((lag + 1, tm, cw), F32),
            pltpu.VMEM((tm, cw), F32),
            pltpu.VMEM((tm, cw), F32),
            pltpu.VMEM((3, tm, cw), BF16),
            dma((2 * xc + 1,)), dma((2 * xc + 1,)),
            dma((nc, 2)), dma((nc, 2)), dma((nc, 2)), dma((nc, 2)), dma((nc, 2)), dma((nc, 2)), dma((3,)), dma((3,)),
            dma((npr,)), dma((npr,)), dma((npr,)), dma((npr,)), dma((npr,)), dma((npr,)), dma((npr,)), dma((npr,)),
            dma((nk,)), dma((nk,)), dma((no,)), dma((no,)), dma((3,)), dma((9,)),
        ],
        compiler_params=pltpu.CompilerParams(
            collective_id=0, has_side_effects=True, vmem_limit_bytes=62 * 1024 * 1024),
    )


def solution(mesh):
    x_spec = P(("grp", "dx", "dz"), "dy")
    w_in_spec = P("dy", ("dz", "dx"))
    w_out_spec = P("dz", ("dy", "dx"))

    def local_mlp(x_blk, wg_blk, wu_blk, wd_blk):
        return make_local_mlp(x_blk.shape, wg_blk.shape, wd_blk.shape)(x_blk, wg_blk, wu_blk, wd_blk)[0]

    return jax.shard_map(local_mlp, mesh=mesh, in_specs=(x_spec, w_in_spec, w_in_spec, w_out_spec), out_specs=x_spec, check_vma=False)
```

```python
import jax
import jax.numpy as jnp
from jax import lax
from jax.experimental import pallas as pl
from jax.experimental.pallas import tpu as pltpu
from jax.sharding import PartitionSpec as P

MESH = pl.DeviceIdType.MESH
BF16 = jnp.bfloat16
F32 = jnp.float32


def make_local_mlp(x_shape, w_shape, d_shape):
    rows, dh = x_shape
    fq = w_shape[1]
    fh, dq = d_shape
    ra = rows // 2
    w = 128
    nc = fq // w
    na = 4
    la = 8
    cw = 256
    npr = dq // cw
    tm = 512
    nz = ra // tm
    ne = tm
    nl = 2 * npr - 1
    nk = nl + nz * (4 * npr - nl)
    no = nz * 2 * npr
    lag = 3
    xc = 2
    xrc = ra // xc
    own, oth = ra, 0

    def kernel(x, wg, wu, wd,
               z, wdy, wpo, wpx, ddy, dpo, dpx, d2o, d2p, zr,
               xg, h, h2, wbuf, dbuf, zs, zin, zacc, zo,
               xs, xr, wys, wyr, wfs, wfr, hs, hr, bs, br,
               dys, dyr, dfs, dfr, d2s, d2r, d2t, d2u,
               zss, zsr, zos, zor, zls, lds):
        dz = lax.axis_index("dz")
        dy = lax.axis_index("dy")
        dx = lax.axis_index("dx")
        to_dz = {"dz": 1 - dz}
        to_dy = {"dy": 1 - dy}
        to_dx = {"dx": 1 - dx}

        def rcopy(src, dst, ss, rs, dev):
            return pltpu.make_async_remote_copy(
                src_ref=src, dst_ref=dst, send_sem=ss, recv_sem=rs, device_id=dev, device_id_type=MESH)

        mine = pl.multiple_of(dy * ra, ra)
        theirs = pl.multiple_of((1 - dy) * ra, ra)
        left, right = pl.ds(0, dh), pl.ds(dh, dh)

        def x_dy(i):
            return rcopy(x.at[pl.ds(theirs + i * xrc, xrc)], xg.at[pl.ds(own + i * xrc, xrc), right],
                         xs.at[i], xr.at[i], to_dy)

        def x_fw(i):
            return rcopy(xg.at[pl.ds(own + i * xrc, xrc), right], xg.at[pl.ds(oth + i * xrc, xrc), right],
                         xs.at[xc + i], xr.at[xc + i], to_dz)

        x_dz = rcopy(x.at[pl.ds(mine, ra)], xg.at[pl.ds(oth, ra), left], xs.at[2 * xc], xr.at[2 * xc], to_dz)
        x_lo = pltpu.make_async_copy(x.at[pl.ds(mine, ra)], xg.at[pl.ds(own, ra), left], lds.at[8])

        def cols(j):
            return pl.ds(pl.multiple_of(j * w, w), w)

        def w_dy(j):
            return [rcopy(src.at[:, cols(j)], wdy.at[j, t], wys.at[j, t], wyr.at[j, t], to_dy)
                    for t, src in enumerate((wg, wu))]

        def w_fw(j):
            return [rcopy(wdy.at[j, t], wpx.at[j, t], wfs.at[j, t], wfr.at[j, t], to_dx) for t in range(2)]

        def dcols(p):
            return pl.ds(pl.multiple_of(p * cw, cw), cw)

        def d_dy(p):
            return rcopy(wd.at[:, dcols(p)], ddy.at[p], dys.at[p], dyr.at[p], to_dy)

        def d_fw(p):
            return rcopy(ddy.at[p], dpx.at[p], dfs.at[p], dfr.at[p], to_dx)

        bulk = [rcopy(src, dst, bs.at[i], br.at[i], to_dx)
                for i, (src, dst) in enumerate(((wg, wpo.at[0]), (wu, wpo.at[1]), (wd, dpo)))]

        def d2_dz(p):
            return rcopy(wd.at[:, dcols(p)], d2o.at[p], d2s.at[p], d2r.at[p], to_dz)

        def d2_fw(p):
            return rcopy(d2o.at[p], d2p.at[p], d2t.at[p], d2u.at[p], to_dx)

        def hcols(j, t):
            return pl.ds(pl.multiple_of(((dx + t) % 2) * fq + j * w, w), w)

        def h_dz(j, t):
            return rcopy(h.at[pl.ds(oth, ne), hcols(j, t)], h2.at[:, hcols(j, t)], hs.at[j, t], hr.at[j, t], to_dz)

        def start(cs):
            for c in cs:
                c.start()

        def wait_all(cs):
            for c in cs:
                c.wait()

        def wait_recv(cs):
            for c in cs:
                c.wait_recv()

        barrier = pltpu.get_barrier_semaphore()
        for dev in (to_dx, to_dy, to_dz):
            pl.semaphore_signal(barrier, inc=1, device_id=dev, device_id_type=MESH)
        pl.semaphore_wait(barrier, 3)

        for i in range(xc):
            x_dy(i).start()
        x_dz.start()
        x_lo.start()
        start(bulk[:2])

        @pl.loop(0, la)
        def _(j):
            start(w_dy(j))

        for i in range(xc):
            x_dy(i).wait_recv()
            x_fw(i).start()
        for p in range(npr - 1):
            d2_dz(p).start()

        @pl.when(dx == 0)
        def _():
            d2_dz(npr - 1).start()

        bulk[2].start()
        x_lo.wait()
        first_d = pltpu.make_async_copy(wd.at[:, dcols(0)], dbuf.at[0], lds.at[8])
        first_d.start()
        wait_recv(bulk[:2])

        def gate_up(row, j):
            rs = pl.ds(pl.multiple_of(row, tm), tm)
            xt = xg[rs, :]
            g = jnp.dot(xt, wbuf[0], preferred_element_type=F32).astype(BF16).astype(F32)
            u = jnp.dot(xt, wbuf[1], preferred_element_type=F32).astype(BF16).astype(F32)
            val = (g * jax.nn.sigmoid(g) * u).astype(BF16)
            for t in range(2):
                h[rs, hcols(j, t)] = val[:, t * w:(t + 1) * w]

        def rest(j):
            @pl.loop(0, nz + 1)
            def _(i):
                gate_up((i + (i + nz) // (nz + 1)) * tm, j)

                @pl.when(i == 1)
                def _():
                    h_dz(j, 0).start()
                    h_dz(j, 1).start()

        lc, rc = pl.ds(0, w), pl.ds(w, w)

        def loads(j):
            return [pltpu.make_async_copy(wg.at[:, cols(j)], wbuf.at[0, left, lc], lds.at[0]),
                    pltpu.make_async_copy(wu.at[:, cols(j)], wbuf.at[1, left, lc], lds.at[1]),
                    pltpu.make_async_copy(wpo.at[0, :, cols(j)], wbuf.at[0, left, rc], lds.at[2]),
                    pltpu.make_async_copy(wpo.at[1, :, cols(j)], wbuf.at[1, left, rc], lds.at[3]),
                    pltpu.make_async_copy(wdy.at[j, 0], wbuf.at[0, right, lc], lds.at[4]),
                    pltpu.make_async_copy(wdy.at[j, 1], wbuf.at[1, right, lc], lds.at[5]),
                    pltpu.make_async_copy(wpx.at[j, 0], wbuf.at[0, right, rc], lds.at[6]),
                    pltpu.make_async_copy(wpx.at[j, 1], wbuf.at[1, right, rc], lds.at[7])]

        def arrive(j):
            @pl.when(j + la < nc)
            def _():
                start(w_dy(j + la))

            wait_recv(w_dy(j))
            start(w_fw(j))
            ld = loads(j)
            start(ld[:6])
            wait_recv(w_fw(j))
            start(ld[6:])
            wait_all(ld)

        @pl.loop(0, na)
        def _(j):
            arrive(j)

            @pl.loop(0, nz)
            def _(i):
                gate_up(own + i * tm, j)

        x_dz.wait_recv()
        for i in range(xc):
            x_fw(i).wait_recv()

        @pl.loop(0, na)
        def _(j):
            ld = loads(j)
            start(ld)
            wait_all(ld)

            @pl.loop(0, nz)
            def _(i):
                gate_up(oth + i * tm, j)

            h_dz(j, 0).start()
            h_dz(j, 1).start()

        @pl.loop(na, nc)
        def _(j):
            @pl.when(jnp.logical_and(j >= la, j < la + npr))
            def _():
                d_dy(j - la).start()

            @pl.when(jnp.logical_and(j >= nc - npr - 1, j < nc - 2))
            def _():
                p = j - (nc - npr - 1)
                d2_dz(p).wait_recv()
                d2_fw(p).start()

            @pl.when(jnp.logical_and(dx == 0, j == nc - 2))
            def _():
                d2_dz(npr - 1).wait_recv()
                d2_fw(npr - 1).start()

            arrive(j)
            gate_up(oth + (nz - 1) * tm, j)

            @pl.when(j < nc - 1)
            def _():
                rest(j)

        bulk[2].wait_recv()

        def split(k):
            late = (k + nk - nl) // nk
            s = (k - nl) // nz
            last = s // (2 * npr)
            odd = k // (nl - 1)
            half = late * (1 - last)
            p = (1 - late) * (k // 2) + late * ((1 - last) * (s // 2) + last * (npr - 1))
            q = (1 - late) * ((1 - odd) * (k % 2) + odd * dx) + late * ((1 - last) * (s % 2) + last * (1 - dx))
            r = (1 - late) * (nz - 1) + late * ((k - nl) % nz)
            return half, p, q, r

        def chunk_src(half, p, q):
            if half == 0:
                return (wd, dpo)[q].at[:, dcols(p)]
            return (ddy, dpx)[q].at[p]

        def load_d(k, slot, ok):
            half, p, q, r = split(k)
            ok = jnp.logical_and(ok, jnp.logical_or(k < nl, r == 0))
            for hh in range(2):
                for qq in range(2):
                    @pl.when(jnp.logical_and(ok, jnp.logical_and(half == hh, q == qq)))
                    def _(hh=hh, qq=qq):
                        c = pltpu.make_async_copy(chunk_src(hh, p, qq), dbuf.at[slot], lds.at[slot])
                        c.start()
                        c.wait()

        def z_send(k):
            return rcopy(zs.at[k % (lag + 1)], zr.at[k], zss.at[k], zsr.at[k], to_dz)

        def out_cols(p, q):
            return pl.ds(pl.multiple_of(((dx + q) % 2) * dq + p * cw, cw), cw)

        def out_at(m, base):
            half, p, q, r = split(m)
            return z.at[pl.ds(pl.multiple_of(base + r * tm, tm), tm), out_cols(p, q)]

        def is_other(m):
            return split(m)[0] == 1

        def out_local(m):
            return pltpu.make_async_copy(zo.at[m % 2], out_at(m, mine), zls.at[m % 2])

        def out_remote(m):
            i = m - nl
            return rcopy(zo.at[m % 2], out_at(m, mine), zos.at[i], zor.at[i], to_dy)

        def in_remote(m):
            i = m - nl
            return rcopy(zo.at[m % 2], out_at(m, theirs), zos.at[i], zor.at[i], to_dy)

        def free_out(m):
            @pl.when(is_other(m))
            def _():
                out_remote(m).wait_send()

            @pl.when(jnp.logical_not(is_other(m)))
            def _():
                out_local(m).wait()

        def send_piece(k):
            half, p, q, r = split(k)

            @pl.when(jnp.logical_and(jnp.logical_and(half == 1, q == 1), r == 0))
            def _():
                d_fw(p).wait_recv()

            @pl.when(k == 0)
            def _():
                first_d.wait()

            load_d(k, 0, k > 0)

            @pl.when(k > lag)
            def _():
                z_send(k - lag - 1).wait_send()

            zs[k % (lag + 1)] = jnp.dot(h[pl.ds(pl.multiple_of(oth + r * tm, tm), tm), :], dbuf[0],
                                        preferred_element_type=F32)
            z_send(k).start()

        def e_out(e):
            _, p, q, _ = split(e)
            return pltpu.make_async_copy(zo.at[2], z.at[pl.ds(mine, ne), out_cols(p, q)], zls.at[2])

        def e_piece(e):
            _, p, q, _ = split(e)
            for qq in range(2):
                @pl.when(q == qq)
                def _(qq=qq):
                    c = [pltpu.make_async_copy(chunk_src(0, p, qq), dbuf.at[2], lds.at[2]),
                         pltpu.make_async_copy((d2o, d2p)[qq].at[p], dbuf.at[3], lds.at[3])]
                    start(c)
                    wait_all(c)

            acc = jnp.dot(h[pl.ds(own, ne), :], dbuf[2], preferred_element_type=F32)
            acc = acc + jnp.dot(h2[...], dbuf[3], preferred_element_type=F32)

            @pl.when(e >= 1)
            def _():
                e_out(e - 1).wait()

            zo[2] = acc.astype(BF16)
            e_out(e).start()

        e0 = 7

        @pl.loop(0, nk + lag)
        def _(k):
            @pl.when(k < nk)
            def _():
                send_piece(k)

            @pl.when(k == lag - 1)
            def _():
                rest(nc - 1)

            f = k - (nl - 1)

            @pl.when(jnp.logical_and(f >= 0, jnp.logical_and(f < 2 * nz * npr, f % (2 * nz) == 0)))
            def _():
                d_dy(f // (2 * nz)).wait_recv()
                d_fw(f // (2 * nz)).start()

            @pl.when(k == e0 - 1)
            def _():
                for p in range(npr - 1):
                    d2_fw(p).wait_recv()

                @pl.when(dx == 1)
                def _():
                    d2_fw(npr - 1).wait_recv()

                @pl.loop(0, nc)
                def _(j):
                    for t in range(2):
                        h_dz(j, t).wait_recv()

            @pl.when(jnp.logical_and(k >= e0, jnp.logical_and(k < e0 + 2 * nl, (k - e0) % 2 == 0)))
            def _():
                e_piece((k - e0) // 2)

            @pl.when(k >= lag)
            def _():
                m = k - lag
                half, p, q, r = split(m)
                load_d(m, 1, k >= lag)
                zacc[...] = jnp.dot(h[pl.ds(pl.multiple_of(own + r * tm, tm), tm), :], dbuf[1],
                                    preferred_element_type=F32)

                @pl.when(m >= 2)
                def _():
                    free_out(m - 2)

                z_send(m).wait_recv()
                c = pltpu.make_async_copy(zr.at[m], zin, lds.at[4])
                c.start()
                c.wait()
                zo[m % 2] = (zacc[...] + zin[...]).astype(BF16)

                @pl.when(half == 0)
                def _():
                    out_local(m).start()

                @pl.when(half == 1)
                def _():
                    out_remote(m).start()

        for m in (nk - 2, nk - 1):
            out_local(m).wait()
        e_out(nl - 1).wait()
        for k in range(nk - lag - 1, nk):
            z_send(k).wait_send()
        for i in range(xc):
            x_dy(i).wait_send()
            x_fw(i).wait_send()
        x_dz.wait_send()

        @pl.loop(0, nc)
        def _(j):
            for c in w_dy(j) + w_fw(j) + [h_dz(j, 0), h_dz(j, 1)]:
                c.wait_send()

        @pl.loop(0, npr)
        def _(p):
            d_dy(p).wait_send()
            d_fw(p).wait_send()

        for c in bulk:
            c.wait_send()
        for p in range(npr - 1):
            d2_dz(p).wait_send()
            d2_fw(p).wait_send()

        @pl.when(dx == 0)
        def _():
            d2_dz(npr - 1).wait_send()
            d2_fw(npr - 1).wait_send()

        @pl.loop(nl, nl + no)
        def _(m):
            in_remote(m).wait_recv()

    def sd(shape, dtype=BF16):
        return jax.ShapeDtypeStruct(shape, dtype)

    wl, dl = sd((nc, 2, dh, w)), sd((npr, fh, cw))
    outs = (sd((rows, dh)), wl, sd((2, dh, fq)), wl, dl, sd((fh, dq)), dl, dl, dl, sd((nk, tm, cw), F32))
    dma = pltpu.SemaphoreType.DMA
    return pl.pallas_call(
        kernel,
        out_shape=outs,
        in_specs=[pl.BlockSpec(memory_space=pl.ANY)] * 4,
        out_specs=[pl.BlockSpec(memory_space=pl.ANY)] * len(outs),
        scratch_shapes=[
            pltpu.VMEM((rows, 2 * dh), BF16),
            pltpu.VMEM((rows, fh), BF16),
            pltpu.VMEM((ne, fh), BF16),
            pltpu.VMEM((2, 2 * dh, 2 * w), BF16),
            pltpu.VMEM((4, fh, cw), BF16),
            pltpu.VMEM((lag + 1, tm, cw), F32),
            pltpu.VMEM((tm, cw), F32),
            pltpu.VMEM((tm, cw), F32),
            pltpu.VMEM((3, tm, cw), BF16),
            dma((2 * xc + 1,)), dma((2 * xc + 1,)),
            dma((nc, 2)), dma((nc, 2)), dma((nc, 2)), dma((nc, 2)), dma((nc, 2)), dma((nc, 2)), dma((3,)), dma((3,)),
            dma((npr,)), dma((npr,)), dma((npr,)), dma((npr,)), dma((npr,)), dma((npr,)), dma((npr,)), dma((npr,)),
            dma((nk,)), dma((nk,)), dma((no,)), dma((no,)), dma((3,)), dma((9,)),
        ],
        compiler_params=pltpu.CompilerParams(
            collective_id=0, has_side_effects=True, vmem_limit_bytes=62 * 1024 * 1024),
    )


def solution(mesh):
    x_spec = P(("grp", "dx", "dz"), "dy")
    w_in_spec = P("dy", ("dz", "dx"))
    w_out_spec = P("dz", ("dy", "dx"))

    def local_mlp(x_blk, wg_blk, wu_blk, wd_blk):
        return make_local_mlp(x_blk.shape, wg_blk.shape, wd_blk.shape)(x_blk, wg_blk, wu_blk, wd_blk)[0]

    return jax.shard_map(local_mlp, mesh=mesh, in_specs=(x_spec, w_in_spec, w_in_spec, w_out_spec), out_specs=x_spec, check_vma=False)
```

```python
import jax
import jax.numpy as jnp
from jax import lax
from jax.experimental import pallas as pl
from jax.experimental.pallas import tpu as pltpu
from jax.sharding import PartitionSpec as P

MESH = pl.DeviceIdType.MESH
BF16 = jnp.bfloat16
F32 = jnp.float32


def make_local_mlp(x_shape, w_shape, d_shape):
    rows, dh = x_shape
    fq = w_shape[1]
    fh, dq = d_shape
    ra = rows // 2
    w = 128
    nc = fq // w
    na = 4
    la = 8
    cw = 256
    npr = dq // cw
    tm = 512
    nz = ra // tm
    ne = tm
    nl = 2 * npr - 1
    nk = nl + nz * (4 * npr - nl)
    no = nz * 2 * npr
    lag = 4
    oslots = 8
    xc = 2
    xrc = ra // xc
    own, oth = ra, 0

    def kernel(x, wg, wu, wd,
               z, wdy, wpo, wpx, ddy, dpo, dpx, d2o, d2p,
               xg, h, h2, wbuf, dbuf, zs, zr, zacc, zo,
               xs, xr, wys, wyr, wfs, wfr, hs, hr, bs, br,
               dys, dyr, dfs, dfr, d2s, d2r, d2t, d2u,
               zss, zsr, zos, zor, zls, lds):
        dz = lax.axis_index("dz")
        dy = lax.axis_index("dy")
        dx = lax.axis_index("dx")
        to_dz = {"dz": 1 - dz}
        to_dy = {"dy": 1 - dy}
        to_dx = {"dx": 1 - dx}

        def rcopy(src, dst, ss, rs, dev):
            return pltpu.make_async_remote_copy(
                src_ref=src, dst_ref=dst, send_sem=ss, recv_sem=rs, device_id=dev, device_id_type=MESH)

        mine = pl.multiple_of(dy * ra, ra)
        theirs = pl.multiple_of((1 - dy) * ra, ra)
        left, right = pl.ds(0, dh), pl.ds(dh, dh)

        def x_dy(i):
            return rcopy(x.at[pl.ds(theirs + i * xrc, xrc)], xg.at[pl.ds(own + i * xrc, xrc), right],
                         xs.at[i], xr.at[i], to_dy)

        def x_fw(i):
            return rcopy(xg.at[pl.ds(own + i * xrc, xrc), right], xg.at[pl.ds(oth + i * xrc, xrc), right],
                         xs.at[xc + i], xr.at[xc + i], to_dz)

        x_dz = rcopy(x.at[pl.ds(mine, ra)], xg.at[pl.ds(oth, ra), left], xs.at[2 * xc], xr.at[2 * xc], to_dz)
        x_lo = pltpu.make_async_copy(x.at[pl.ds(mine, ra)], xg.at[pl.ds(own, ra), left], lds.at[8])

        def cols(j):
            return pl.ds(pl.multiple_of(j * w, w), w)

        def w_dy(j):
            return [rcopy(src.at[:, cols(j)], wdy.at[j, t], wys.at[j, t], wyr.at[j, t], to_dy)
                    for t, src in enumerate((wg, wu))]

        def w_fw(j):
            return [rcopy(wdy.at[j, t], wpx.at[j, t], wfs.at[j, t], wfr.at[j, t], to_dx) for t in range(2)]

        def dcols(p):
            return pl.ds(pl.multiple_of(p * cw, cw), cw)

        def d_dy(p):
            return rcopy(wd.at[:, dcols(p)], ddy.at[p], dys.at[p], dyr.at[p], to_dy)

        def d_fw(p):
            return rcopy(ddy.at[p], dpx.at[p], dfs.at[p], dfr.at[p], to_dx)

        bulk = [rcopy(src, dst, bs.at[i], br.at[i], to_dx)
                for i, (src, dst) in enumerate(((wg, wpo.at[0]), (wu, wpo.at[1]), (wd, dpo)))]

        def d2_dz(p):
            return rcopy(wd.at[:, dcols(p)], d2o.at[p], d2s.at[p], d2r.at[p], to_dz)

        def d2_fw(p):
            return rcopy(d2o.at[p], d2p.at[p], d2t.at[p], d2u.at[p], to_dx)

        def hcols(j, t):
            return pl.ds(pl.multiple_of(((dx + t) % 2) * fq + j * w, w), w)

        def h_dz(j, t):
            return rcopy(h.at[pl.ds(oth, ne), hcols(j, t)], h2.at[:, hcols(j, t)], hs.at[j, t], hr.at[j, t], to_dz)

        def start(cs):
            for c in cs:
                c.start()

        def wait_all(cs):
            for c in cs:
                c.wait()

        def wait_recv(cs):
            for c in cs:
                c.wait_recv()

        barrier = pltpu.get_barrier_semaphore()
        for dev in (to_dx, to_dy, to_dz):
            pl.semaphore_signal(barrier, inc=1, device_id=dev, device_id_type=MESH)
        pl.semaphore_wait(barrier, 3)

        for i in range(xc):
            x_dy(i).start()
        x_dz.start()
        x_lo.start()
        start(bulk[:2])

        @pl.loop(0, la)
        def _(j):
            start(w_dy(j))

        for i in range(xc):
            x_dy(i).wait_recv()
            x_fw(i).start()
        for p in range(npr - 1):
            d2_dz(p).start()

        @pl.when(dx == 0)
        def _():
            d2_dz(npr - 1).start()

        bulk[2].start()
        x_lo.wait()
        first_d = pltpu.make_async_copy(wd.at[:, dcols(0)], dbuf.at[0], lds.at[8])
        first_d.start()
        wait_recv(bulk[:2])

        def gate_up(row, j):
            rs = pl.ds(pl.multiple_of(row, tm), tm)
            xt = xg[rs, :]
            g = jnp.dot(xt, wbuf[0], preferred_element_type=F32).astype(BF16).astype(F32)
            u = jnp.dot(xt, wbuf[1], preferred_element_type=F32).astype(BF16).astype(F32)
            val = (g * jax.nn.sigmoid(g) * u).astype(BF16)
            for t in range(2):
                h[rs, hcols(j, t)] = val[:, t * w:(t + 1) * w]

        def rest(j):
            @pl.loop(0, nz + 1)
            def _(i):
                gate_up((i + (i + nz) // (nz + 1)) * tm, j)

                @pl.when(i == 1)
                def _():
                    h_dz(j, 0).start()
                    h_dz(j, 1).start()

        lc, rc = pl.ds(0, w), pl.ds(w, w)

        def loads(j):
            return [pltpu.make_async_copy(wg.at[:, cols(j)], wbuf.at[0, left, lc], lds.at[0]),
                    pltpu.make_async_copy(wu.at[:, cols(j)], wbuf.at[1, left, lc], lds.at[1]),
                    pltpu.make_async_copy(wpo.at[0, :, cols(j)], wbuf.at[0, left, rc], lds.at[2]),
                    pltpu.make_async_copy(wpo.at[1, :, cols(j)], wbuf.at[1, left, rc], lds.at[3]),
                    pltpu.make_async_copy(wdy.at[j, 0], wbuf.at[0, right, lc], lds.at[4]),
                    pltpu.make_async_copy(wdy.at[j, 1], wbuf.at[1, right, lc], lds.at[5]),
                    pltpu.make_async_copy(wpx.at[j, 0], wbuf.at[0, right, rc], lds.at[6]),
                    pltpu.make_async_copy(wpx.at[j, 1], wbuf.at[1, right, rc], lds.at[7])]

        def arrive(j):
            @pl.when(j + la < nc)
            def _():
                start(w_dy(j + la))

            wait_recv(w_dy(j))
            start(w_fw(j))
            ld = loads(j)
            start(ld[:6])
            wait_recv(w_fw(j))
            start(ld[6:])
            wait_all(ld)

        @pl.loop(0, na)
        def _(j):
            arrive(j)

            @pl.loop(0, nz)
            def _(i):
                gate_up(own + i * tm, j)

        x_dz.wait_recv()
        for i in range(xc):
            x_fw(i).wait_recv()

        @pl.loop(0, na)
        def _(j):
            ld = loads(j)
            start(ld)
            wait_all(ld)

            @pl.loop(0, nz)
            def _(i):
                gate_up(oth + i * tm, j)

            h_dz(j, 0).start()
            h_dz(j, 1).start()

        @pl.loop(na, nc)
        def _(j):
            @pl.when(jnp.logical_and(j >= la, j < la + npr))
            def _():
                d_dy(j - la).start()

            @pl.when(jnp.logical_and(j >= nc - npr - 1, j < nc - 2))
            def _():
                p = j - (nc - npr - 1)
                d2_dz(p).wait_recv()
                d2_fw(p).start()

            @pl.when(jnp.logical_and(dx == 0, j == nc - 2))
            def _():
                d2_dz(npr - 1).wait_recv()
                d2_fw(npr - 1).start()

            arrive(j)
            gate_up(oth + (nz - 1) * tm, j)

            @pl.when(j < nc - 1)
            def _():
                rest(j)

        bulk[2].wait_recv()

        def split(k):
            late = (k + nk - nl) // nk
            s = (k - nl) // nz
            last = s // (2 * npr)
            odd = k // (nl - 1)
            half = late * (1 - last)
            p = (1 - late) * (k // 2) + late * ((1 - last) * (s // 2) + last * (npr - 1))
            q = (1 - late) * ((1 - odd) * (k % 2) + odd * dx) + late * ((1 - last) * (s % 2) + last * (1 - dx))
            r = (1 - late) * (nz - 1) + late * ((k - nl) % nz)
            return half, p, q, r

        def chunk_src(half, p, q):
            if half == 0:
                return (wd, dpo)[q].at[:, dcols(p)]
            return (ddy, dpx)[q].at[p]

        def load_d(k, slot, ok):
            half, p, q, r = split(k)
            ok = jnp.logical_and(ok, jnp.logical_or(k < nl, r == 0))
            for hh in range(2):
                for qq in range(2):
                    @pl.when(jnp.logical_and(ok, jnp.logical_and(half == hh, q == qq)))
                    def _(hh=hh, qq=qq):
                        c = pltpu.make_async_copy(chunk_src(hh, p, qq), dbuf.at[slot], lds.at[slot])
                        c.start()
                        c.wait()

        def z_send(k):
            return rcopy(zs.at[k % (lag + 1)], zr.at[k], zss.at[k], zsr.at[k], to_dz)

        def out_cols(p, q):
            return pl.ds(pl.multiple_of(((dx + q) % 2) * dq + p * cw, cw), cw)

        def out_at(m, base):
            half, p, q, r = split(m)
            return z.at[pl.ds(pl.multiple_of(base + r * tm, tm), tm), out_cols(p, q)]

        def is_other(m):
            return split(m)[0] == 1

        def out_local(m):
            return pltpu.make_async_copy(zo.at[m % oslots], out_at(m, mine), zls.at[m % oslots])

        def out_remote(m):
            i = m - nl
            return rcopy(zo.at[m % oslots], out_at(m, mine), zos.at[i], zor.at[i], to_dy)

        def in_remote(m):
            i = m - nl
            return rcopy(zo.at[m % oslots], out_at(m, theirs), zos.at[i], zor.at[i], to_dy)

        def free_out(m):
            @pl.when(is_other(m))
            def _():
                out_remote(m).wait_send()

            @pl.when(jnp.logical_not(is_other(m)))
            def _():
                out_local(m).wait()

        def send_piece(k):
            half, p, q, r = split(k)

            @pl.when(jnp.logical_and(jnp.logical_and(half == 1, q == 1), r == 0))
            def _():
                d_fw(p).wait_recv()

            @pl.when(k == 0)
            def _():
                first_d.wait()

            load_d(k, 0, k > 0)

            @pl.when(k > lag)
            def _():
                z_send(k - lag - 1).wait_send()

            zs[k % (lag + 1)] = jnp.dot(h[pl.ds(pl.multiple_of(oth + r * tm, tm), tm), :], dbuf[0],
                                        preferred_element_type=F32)
            z_send(k).start()

        def e_out(e):
            _, p, q, _ = split(e)
            return pltpu.make_async_copy(zo.at[oslots], z.at[pl.ds(mine, ne), out_cols(p, q)], zls.at[oslots])

        def e_piece(e):
            _, p, q, _ = split(e)
            for qq in range(2):
                @pl.when(q == qq)
                def _(qq=qq):
                    c = [pltpu.make_async_copy(chunk_src(0, p, qq), dbuf.at[2], lds.at[2]),
                         pltpu.make_async_copy((d2o, d2p)[qq].at[p], dbuf.at[3], lds.at[3])]
                    start(c)
                    wait_all(c)

            acc = jnp.dot(h[pl.ds(own, ne), :], dbuf[2], preferred_element_type=F32)
            acc = acc + jnp.dot(h2[...], dbuf[3], preferred_element_type=F32)

            @pl.when(e >= 1)
            def _():
                e_out(e - 1).wait()

            zo[oslots] = acc.astype(BF16)
            e_out(e).start()

        e0 = 7

        @pl.loop(0, nk + lag)
        def _(k):
            @pl.when(k < nk)
            def _():
                send_piece(k)

            @pl.when(k == lag - 1)
            def _():
                rest(nc - 1)

            f = k - (nl - 1)

            @pl.when(jnp.logical_and(f >= 0, jnp.logical_and(f < 2 * nz * npr, f % (2 * nz) == 0)))
            def _():
                d_dy(f // (2 * nz)).wait_recv()
                d_fw(f // (2 * nz)).start()

            @pl.when(k == e0 - 1)
            def _():
                for p in range(npr - 1):
                    d2_fw(p).wait_recv()

                @pl.when(dx == 1)
                def _():
                    d2_fw(npr - 1).wait_recv()

                @pl.loop(0, nc)
                def _(j):
                    for t in range(2):
                        h_dz(j, t).wait_recv()

            @pl.when(jnp.logical_and(k >= e0, jnp.logical_and(k < e0 + 2 * nl, (k - e0) % 2 == 0)))
            def _():
                e_piece((k - e0) // 2)

            @pl.when(k >= lag)
            def _():
                m = k - lag
                half, p, q, r = split(m)
                load_d(m, 1, k >= lag)
                zacc[...] = jnp.dot(h[pl.ds(pl.multiple_of(own + r * tm, tm), tm), :], dbuf[1],
                                    preferred_element_type=F32)

                @pl.when(m >= oslots)
                def _():
                    free_out(m - oslots)

                z_send(m).wait_recv()
                zo[m % oslots] = (zacc[...] + zr[m]).astype(BF16)

                @pl.when(half == 0)
                def _():
                    out_local(m).start()

                @pl.when(half == 1)
                def _():
                    out_remote(m).start()

        @pl.loop(nk - oslots, nk)
        def _(m):
            free_out(m)

        e_out(nl - 1).wait()
        for k in range(nk - lag - 1, nk):
            z_send(k).wait_send()
        for i in range(xc):
            x_dy(i).wait_send()
            x_fw(i).wait_send()
        x_dz.wait_send()

        @pl.loop(0, nc)
        def _(j):
            for c in w_dy(j) + w_fw(j) + [h_dz(j, 0), h_dz(j, 1)]:
                c.wait_send()

        @pl.loop(0, npr)
        def _(p):
            d_dy(p).wait_send()
            d_fw(p).wait_send()

        for c in bulk:
            c.wait_send()
        for p in range(npr - 1):
            d2_dz(p).wait_send()
            d2_fw(p).wait_send()

        @pl.when(dx == 0)
        def _():
            d2_dz(npr - 1).wait_send()
            d2_fw(npr - 1).wait_send()

        @pl.loop(nl, nl + no)
        def _(m):
            in_remote(m).wait_recv()

    def sd(shape, dtype=BF16):
        return jax.ShapeDtypeStruct(shape, dtype)

    wl, dl = sd((nc, 2, dh, w)), sd((npr, fh, cw))
    outs = (sd((rows, dh)), wl, sd((2, dh, fq)), wl, dl, sd((fh, dq)), dl, dl, dl)
    dma = pltpu.SemaphoreType.DMA
    return pl.pallas_call(
        kernel,
        out_shape=outs,
        in_specs=[pl.BlockSpec(memory_space=pl.ANY)] * 4,
        out_specs=[pl.BlockSpec(memory_space=pl.ANY)] * len(outs),
        scratch_shapes=[
            pltpu.VMEM((rows, 2 * dh), BF16),
            pltpu.VMEM((rows, fh), BF16),
            pltpu.VMEM((ne, fh), BF16),
            pltpu.VMEM((2, 2 * dh, 2 * w), BF16),
            pltpu.VMEM((4, fh, cw), BF16),
            pltpu.VMEM((lag + 1, tm, cw), F32),
            pltpu.VMEM((nk, tm, cw), F32),
            pltpu.VMEM((tm, cw), F32),
            pltpu.VMEM((oslots + 1, tm, cw), BF16),
            dma((2 * xc + 1,)), dma((2 * xc + 1,)),
            dma((nc, 2)), dma((nc, 2)), dma((nc, 2)), dma((nc, 2)), dma((nc, 2)), dma((nc, 2)), dma((3,)), dma((3,)),
            dma((npr,)), dma((npr,)), dma((npr,)), dma((npr,)), dma((npr,)), dma((npr,)), dma((npr,)), dma((npr,)),
            dma((nk,)), dma((nk,)), dma((no,)), dma((no,)), dma((oslots + 1,)), dma((9,)),
        ],
        compiler_params=pltpu.CompilerParams(
            collective_id=0, has_side_effects=True, vmem_limit_bytes=62 * 1024 * 1024),
    )


def solution(mesh):
    x_spec = P(("grp", "dx", "dz"), "dy")
    w_in_spec = P("dy", ("dz", "dx"))
    w_out_spec = P("dz", ("dy", "dx"))

    def local_mlp(x_blk, wg_blk, wu_blk, wd_blk):
        return make_local_mlp(x_blk.shape, wg_blk.shape, wd_blk.shape)(x_blk, wg_blk, wu_blk, wd_blk)[0]

    return jax.shard_map(local_mlp, mesh=mesh, in_specs=(x_spec, w_in_spec, w_in_spec, w_out_spec), out_specs=x_spec, check_vma=False)
```

```python
import jax
import jax.numpy as jnp
from jax import lax
from jax.experimental import pallas as pl
from jax.experimental.pallas import tpu as pltpu
from jax.sharding import PartitionSpec as P

MESH = pl.DeviceIdType.MESH
BF16 = jnp.bfloat16
F32 = jnp.float32


def make_local_mlp(x_shape, w_shape, d_shape):
    rows, dh = x_shape
    fq = w_shape[1]
    fh, dq = d_shape
    ra = rows // 2
    w = 128
    nc = fq // w
    na = 4
    la = 8
    cw = 256
    npr = dq // cw
    tm = 512
    nz = ra // tm
    ne = tm + 64
    nn = ra - ne
    nl = 2 * npr - 1
    nk = nl + nz * (4 * npr - nl)
    no = nz * 2 * npr
    lag = 4
    oslots = 8
    xc = 2
    xrc = ra // xc
    own, oth = ra, 0

    def kernel(x, wg, wu, wd,
               z, wdy, wpo, wpx, ddy, dpo, dpx, d2o, d2p,
               xg, h, h2, wbuf, wlast, dbuf, zs, zr, zacc, zo, zoe,
               xs, xr, wys, wyr, wfs, wfr, hs, hr, bs, br,
               dys, dyr, dfs, dfr, d2s, d2r, d2t, d2u,
               zss, zsr, zos, zor, zls, lds):
        dz = lax.axis_index("dz")
        dy = lax.axis_index("dy")
        dx = lax.axis_index("dx")
        to_dz = {"dz": 1 - dz}
        to_dy = {"dy": 1 - dy}
        to_dx = {"dx": 1 - dx}

        def rcopy(src, dst, ss, rs, dev):
            return pltpu.make_async_remote_copy(
                src_ref=src, dst_ref=dst, send_sem=ss, recv_sem=rs, device_id=dev, device_id_type=MESH)

        mine = pl.multiple_of(dy * ra, ra)
        theirs = pl.multiple_of((1 - dy) * ra, ra)
        left, right = pl.ds(0, dh), pl.ds(dh, dh)

        def x_dy(i):
            return rcopy(x.at[pl.ds(theirs + i * xrc, xrc)], xg.at[pl.ds(own + i * xrc, xrc), right],
                         xs.at[i], xr.at[i], to_dy)

        def x_fw(i):
            return rcopy(xg.at[pl.ds(own + i * xrc, xrc), right], xg.at[pl.ds(oth + i * xrc, xrc), right],
                         xs.at[xc + i], xr.at[xc + i], to_dz)

        x_dz = rcopy(x.at[pl.ds(mine, ra)], xg.at[pl.ds(oth, ra), left], xs.at[2 * xc], xr.at[2 * xc], to_dz)
        x_lo = pltpu.make_async_copy(x.at[pl.ds(mine, ra)], xg.at[pl.ds(own, ra), left], lds.at[8])

        def cols(j):
            return pl.ds(pl.multiple_of(j * w, w), w)

        def w_dy(j):
            return [rcopy(src.at[:, cols(j)], wdy.at[j, t], wys.at[j, t], wyr.at[j, t], to_dy)
                    for t, src in enumerate((wg, wu))]

        def w_fw(j):
            return [rcopy(wdy.at[j, t], wpx.at[j, t], wfs.at[j, t], wfr.at[j, t], to_dx) for t in range(2)]

        lc, rc = pl.ds(0, w), pl.ds(w, w)
        jl = nc - 1
        w_dy_last = [rcopy(src.at[:, pl.ds(jl * w, w)], wlast.at[t, right, lc], wys.at[jl, t], wyr.at[jl, t], to_dy)
                     for t, src in enumerate((wg, wu))]
        w_fw_last = [rcopy(wlast.at[t, right, lc], wlast.at[t, right, rc], wfs.at[jl, t], wfr.at[jl, t], to_dx)
                     for t in range(2)]
        ld_last = [pltpu.make_async_copy(src.at[:, pl.ds(jl * w, w)], wlast.at[t, left, c], lds.at[9 + 2 * i + t])
                   for i, (srcs, c) in enumerate((((wg, wu), lc), ((wpo.at[0], wpo.at[1]), rc)))
                   for t, src in enumerate(srcs)]

        def dcols(p):
            return pl.ds(pl.multiple_of(p * cw, cw), cw)

        def d_dy(p):
            return rcopy(wd.at[:, dcols(p)], ddy.at[p], dys.at[p], dyr.at[p], to_dy)

        def d_fw(p):
            return rcopy(ddy.at[p], dpx.at[p], dfs.at[p], dfr.at[p], to_dx)

        bulk = [rcopy(src, dst, bs.at[i], br.at[i], to_dx)
                for i, (src, dst) in enumerate(((wg, wpo.at[0]), (wu, wpo.at[1]), (wd, dpo)))]

        def d2_dz(p):
            return rcopy(wd.at[:, dcols(p)], d2o.at[p], d2s.at[p], d2r.at[p], to_dz)

        def d2_fw(p):
            return rcopy(d2o.at[p], d2p.at[p], d2t.at[p], d2u.at[p], to_dx)

        def hcols(j, t):
            return pl.ds(pl.multiple_of(((dx + t) % 2) * fq + j * w, w), w)

        def h_dz(j, t):
            return rcopy(h.at[pl.ds(oth, ne), hcols(j, t)], h2.at[:, hcols(j, t)], hs.at[j, t], hr.at[j, t], to_dz)

        def start(cs):
            for c in cs:
                c.start()

        def wait_all(cs):
            for c in cs:
                c.wait()

        def wait_recv(cs):
            for c in cs:
                c.wait_recv()

        barrier = pltpu.get_barrier_semaphore()
        for dev in (to_dx, to_dy, to_dz):
            pl.semaphore_signal(barrier, inc=1, device_id=dev, device_id_type=MESH)
        pl.semaphore_wait(barrier, 3)

        for i in range(xc):
            x_dy(i).start()
        x_dz.start()
        x_lo.start()
        start(bulk[:2])

        @pl.loop(0, la)
        def _(j):
            start(w_dy(j))

        for i in range(xc):
            x_dy(i).wait_recv()
            x_fw(i).start()
        for p in range(npr - 1):
            d2_dz(p).start()

        @pl.when(dx == 0)
        def _():
            d2_dz(npr - 1).start()

        bulk[2].start()
        x_lo.wait()
        first_d = pltpu.make_async_copy(wd.at[:, dcols(0)], dbuf.at[0], lds.at[8])
        first_d.start()
        wait_recv(bulk[:2])

        def gate_up(row, n, j, wb):
            rs = pl.ds(pl.multiple_of(row, 64), n)
            xt = xg[rs, :]
            g = jnp.dot(xt, wb[0], preferred_element_type=F32).astype(BF16).astype(F32)
            u = jnp.dot(xt, wb[1], preferred_element_type=F32).astype(BF16).astype(F32)
            val = (g * jax.nn.sigmoid(g) * u).astype(BF16)
            for t in range(2):
                h[rs, hcols(j, t)] = val[:, t * w:(t + 1) * w]

        def rest(j, wb):
            gate_up(oth, ne, j, wb)

            @pl.loop(0, nz)
            def _(i):
                gate_up(own + i * tm, tm, j, wb)

                @pl.when(i == 0)
                def _():
                    h_dz(j, 0).start()
                    h_dz(j, 1).start()

        def loads(j):
            return [pltpu.make_async_copy(wg.at[:, cols(j)], wbuf.at[0, left, lc], lds.at[0]),
                    pltpu.make_async_copy(wu.at[:, cols(j)], wbuf.at[1, left, lc], lds.at[1]),
                    pltpu.make_async_copy(wpo.at[0, :, cols(j)], wbuf.at[0, left, rc], lds.at[2]),
                    pltpu.make_async_copy(wpo.at[1, :, cols(j)], wbuf.at[1, left, rc], lds.at[3]),
                    pltpu.make_async_copy(wdy.at[j, 0], wbuf.at[0, right, lc], lds.at[4]),
                    pltpu.make_async_copy(wdy.at[j, 1], wbuf.at[1, right, lc], lds.at[5]),
                    pltpu.make_async_copy(wpx.at[j, 0], wbuf.at[0, right, rc], lds.at[6]),
                    pltpu.make_async_copy(wpx.at[j, 1], wbuf.at[1, right, rc], lds.at[7])]

        def arrive(j):
            @pl.when(j + la < jl)
            def _():
                start(w_dy(j + la))

            @pl.when(j + la == jl)
            def _():
                start(w_dy_last)

            wait_recv(w_dy(j))
            start(w_fw(j))
            ld = loads(j)
            start(ld[:6])
            wait_recv(w_fw(j))
            start(ld[6:])
            wait_all(ld)

        @pl.loop(0, na)
        def _(j):
            arrive(j)

            @pl.loop(0, nz)
            def _(i):
                gate_up(own + i * tm, tm, j, wbuf)

        start(ld_last)
        x_dz.wait_recv()
        for i in range(xc):
            x_fw(i).wait_recv()

        @pl.loop(0, na)
        def _(j):
            ld = loads(j)
            start(ld)
            wait_all(ld)

            gate_up(oth, ne, j, wbuf)
            gate_up(oth + ne, nn, j, wbuf)
            h_dz(j, 0).start()
            h_dz(j, 1).start()

        @pl.loop(na, jl)
        def _(j):
            @pl.when(jnp.logical_and(j >= la, j < la + npr))
            def _():
                d_dy(j - la).start()

            @pl.when(jnp.logical_and(j >= nc - npr - 1, j < nc - 2))
            def _():
                p = j - (nc - npr - 1)
                d2_dz(p).wait_recv()
                d2_fw(p).start()

            @pl.when(jnp.logical_and(dx == 0, j == nc - 2))
            def _():
                d2_dz(npr - 1).wait_recv()
                d2_fw(npr - 1).start()

            arrive(j)
            gate_up(oth + ne, nn, j, wbuf)
            rest(j, wbuf)

        wait_all(ld_last)
        wait_recv(w_dy_last)
        start(w_fw_last)
        wait_recv(w_fw_last)
        gate_up(oth + ne, nn, jl, wlast)
        bulk[2].wait_recv()

        def split(k):
            late = (k + nk - nl) // nk
            s = (k - nl) // nz
            last = s // (2 * npr)
            odd = k // (nl - 1)
            half = late * (1 - last)
            p = (1 - late) * (k // 2) + late * ((1 - last) * (s // 2) + last * (npr - 1))
            q = (1 - late) * ((1 - odd) * (k % 2) + odd * dx) + late * ((1 - last) * (s % 2) + last * (1 - dx))
            r = (1 - late) * (nz - 1) + late * ((k - nl) % nz)
            return half, p, q, r

        def chunk_src(half, p, q):
            if half == 0:
                return (wd, dpo)[q].at[:, dcols(p)]
            return (ddy, dpx)[q].at[p]

        def load_d(k, slot, ok):
            half, p, q, r = split(k)
            ok = jnp.logical_and(ok, jnp.logical_or(k < nl, r == 0))
            for hh in range(2):
                for qq in range(2):
                    @pl.when(jnp.logical_and(ok, jnp.logical_and(half == hh, q == qq)))
                    def _(hh=hh, qq=qq):
                        c = pltpu.make_async_copy(chunk_src(hh, p, qq), dbuf.at[slot], lds.at[slot])
                        c.start()
                        c.wait()

        def sized(k, fn):
            _, _, _, r = split(k)

            @pl.when(k < nl)
            def _():
                fn(ne, nn)

            @pl.when(k >= nl)
            def _():
                fn(pl.multiple_of(r * tm, tm), tm)

        def z_send(k, n):
            return rcopy(zs.at[k % (lag + 1), pl.ds(0, n)], zr.at[k, pl.ds(0, n)], zss.at[k], zsr.at[k], to_dz)

        def out_cols(p, q):
            return pl.ds(pl.multiple_of(((dx + q) % 2) * dq + p * cw, cw), cw)

        def out_at(m, base):
            half, p, q, r = split(m)
            return z.at[pl.ds(pl.multiple_of(base + r * tm, tm), tm), out_cols(p, q)]

        def is_other(m):
            return split(m)[0] == 1

        def out_local(m, row, n):
            _, p, q, _ = split(m)
            return pltpu.make_async_copy(zo.at[m % oslots, pl.ds(0, n)],
                                         z.at[pl.ds(pl.multiple_of(mine + row, 64), n), out_cols(p, q)],
                                         zls.at[m % oslots])

        def out_remote(m):
            i = m - nl
            return rcopy(zo.at[m % oslots], out_at(m, mine), zos.at[i], zor.at[i], to_dy)

        def in_remote(m):
            i = m - nl
            return rcopy(zo.at[m % oslots], out_at(m, theirs), zos.at[i], zor.at[i], to_dy)

        def free_out(m):
            @pl.when(is_other(m))
            def _():
                out_remote(m).wait_send()

            @pl.when(jnp.logical_not(is_other(m)))
            def _():
                sized(m, lambda row, n: out_local(m, row, n).wait())

        def send_piece(k):
            half, p, q, r = split(k)

            @pl.when(jnp.logical_and(jnp.logical_and(half == 1, q == 1), r == 0))
            def _():
                d_fw(p).wait_recv()

            @pl.when(k == 0)
            def _():
                first_d.wait()

            load_d(k, 0, k > 0)

            @pl.when(k > lag)
            def _():
                sized(k - lag - 1, lambda row, n: z_send(k - lag - 1, n).wait_send())

            def piece(row, n):
                zs[k % (lag + 1), pl.ds(0, n)] = jnp.dot(h[pl.ds(pl.multiple_of(oth + row, 64), n), :], dbuf[0],
                                                         preferred_element_type=F32)
                z_send(k, n).start()

            sized(k, piece)

        def e_out(e):
            _, p, q, _ = split(e)
            return pltpu.make_async_copy(zoe, z.at[pl.ds(mine, ne), out_cols(p, q)], zls.at[oslots])

        def e_piece(e):
            _, p, q, _ = split(e)
            for qq in range(2):
                @pl.when(q == qq)
                def _(qq=qq):
                    c = [pltpu.make_async_copy(chunk_src(0, p, qq), dbuf.at[2], lds.at[2]),
                         pltpu.make_async_copy((d2o, d2p)[qq].at[p], dbuf.at[3], lds.at[3])]
                    start(c)
                    wait_all(c)

            acc = jnp.dot(h[pl.ds(own, ne), :], dbuf[2], preferred_element_type=F32)
            acc = acc + jnp.dot(h2[...], dbuf[3], preferred_element_type=F32)

            @pl.when(e >= 1)
            def _():
                e_out(e - 1).wait()

            zoe[...] = acc.astype(BF16)
            e_out(e).start()

        e0 = 7

        @pl.loop(0, nk + lag)
        def _(k):
            @pl.when(k < nk)
            def _():
                send_piece(k)

            @pl.when(k == lag - 1)
            def _():
                rest(jl, wlast)

            f = k - (nl - 1)

            @pl.when(jnp.logical_and(f >= 0, jnp.logical_and(f < 2 * nz * npr, f % (2 * nz) == 0)))
            def _():
                d_dy(f // (2 * nz)).wait_recv()
                d_fw(f // (2 * nz)).start()

            @pl.when(k == e0 - 1)
            def _():
                for p in range(npr - 1):
                    d2_fw(p).wait_recv()

                @pl.when(dx == 1)
                def _():
                    d2_fw(npr - 1).wait_recv()

                @pl.loop(0, nc)
                def _(j):
                    for t in range(2):
                        h_dz(j, t).wait_recv()

            @pl.when(jnp.logical_and(k >= e0, jnp.logical_and(k < e0 + 2 * nl, (k - e0) % 2 == 0)))
            def _():
                e_piece((k - e0) // 2)

            @pl.when(k >= lag)
            def _():
                m = k - lag
                half, p, q, r = split(m)
                load_d(m, 1, k >= lag)
                @pl.when(m >= oslots)
                def _():
                    free_out(m - oslots)

                def piece(row, n):
                    zacc[pl.ds(0, n)] = jnp.dot(h[pl.ds(pl.multiple_of(own + row, 64), n), :], dbuf[1],
                                                preferred_element_type=F32)
                    z_send(m, n).wait_recv()
                    zo[m % oslots, pl.ds(0, n)] = (zacc[pl.ds(0, n)] + zr[m, pl.ds(0, n)]).astype(BF16)

                sized(m, piece)

                @pl.when(half == 0)
                def _():
                    sized(m, lambda row, n: out_local(m, row, n).start())

                @pl.when(half == 1)
                def _():
                    out_remote(m).start()

        @pl.loop(nk - oslots, nk)
        def _(m):
            free_out(m)

        e_out(nl - 1).wait()
        for k in range(nk - lag - 1, nk):
            z_send(k, tm).wait_send()
        for i in range(xc):
            x_dy(i).wait_send()
            x_fw(i).wait_send()
        x_dz.wait_send()

        for c in w_dy_last + w_fw_last + [h_dz(jl, 0), h_dz(jl, 1)]:
            c.wait_send()

        @pl.loop(0, jl)
        def _(j):
            for c in w_dy(j) + w_fw(j) + [h_dz(j, 0), h_dz(j, 1)]:
                c.wait_send()

        @pl.loop(0, npr)
        def _(p):
            d_dy(p).wait_send()
            d_fw(p).wait_send()

        for c in bulk:
            c.wait_send()
        for p in range(npr - 1):
            d2_dz(p).wait_send()
            d2_fw(p).wait_send()

        @pl.when(dx == 0)
        def _():
            d2_dz(npr - 1).wait_send()
            d2_fw(npr - 1).wait_send()

        @pl.loop(nl, nl + no)
        def _(m):
            in_remote(m).wait_recv()

    def sd(shape, dtype=BF16):
        return jax.ShapeDtypeStruct(shape, dtype)

    wl, dl = sd((nc, 2, dh, w)), sd((npr, fh, cw))
    outs = (sd((rows, dh)), wl, sd((2, dh, fq)), wl, dl, sd((fh, dq)), dl, dl, dl)
    dma = pltpu.SemaphoreType.DMA
    return pl.pallas_call(
        kernel,
        out_shape=outs,
        in_specs=[pl.BlockSpec(memory_space=pl.ANY)] * 4,
        out_specs=[pl.BlockSpec(memory_space=pl.ANY)] * len(outs),
        scratch_shapes=[
            pltpu.VMEM((rows, 2 * dh), BF16),
            pltpu.VMEM((rows, fh), BF16),
            pltpu.VMEM((ne, fh), BF16),
            pltpu.VMEM((2, 2 * dh, 2 * w), BF16),
            pltpu.VMEM((2, 2 * dh, 2 * w), BF16),
            pltpu.VMEM((4, fh, cw), BF16),
            pltpu.VMEM((lag + 1, tm, cw), F32),
            pltpu.VMEM((nk, tm, cw), F32),
            pltpu.VMEM((tm, cw), F32),
            pltpu.VMEM((oslots, tm, cw), BF16),
            pltpu.VMEM((ne, cw), BF16),
            dma((2 * xc + 1,)), dma((2 * xc + 1,)),
            dma((nc, 2)), dma((nc, 2)), dma((nc, 2)), dma((nc, 2)), dma((nc, 2)), dma((nc, 2)), dma((3,)), dma((3,)),
            dma((npr,)), dma((npr,)), dma((npr,)), dma((npr,)), dma((npr,)), dma((npr,)), dma((npr,)), dma((npr,)),
            dma((nk,)), dma((nk,)), dma((no,)), dma((no,)), dma((oslots + 1,)), dma((13,)),
        ],
        compiler_params=pltpu.CompilerParams(
            collective_id=0, has_side_effects=True, vmem_limit_bytes=67043328),
    )


def solution(mesh):
    x_spec = P(("grp", "dx", "dz"), "dy")
    w_in_spec = P("dy", ("dz", "dx"))
    w_out_spec = P("dz", ("dy", "dx"))

    def local_mlp(x_blk, wg_blk, wu_blk, wd_blk):
        return make_local_mlp(x_blk.shape, wg_blk.shape, wd_blk.shape)(x_blk, wg_blk, wu_blk, wd_blk)[0]

    return jax.shard_map(local_mlp, mesh=mesh, in_specs=(x_spec, w_in_spec, w_in_spec, w_out_spec), out_specs=x_spec, check_vma=False)
```

```python
import jax
import jax.numpy as jnp
from jax import lax
from jax.experimental import pallas as pl
from jax.experimental.pallas import tpu as pltpu
from jax.sharding import PartitionSpec as P

MESH = pl.DeviceIdType.MESH
BF16 = jnp.bfloat16
F32 = jnp.float32


def make_local_mlp(x_shape, w_shape, d_shape):
    rows, dh = x_shape
    fq = w_shape[1]
    fh, dq = d_shape
    ra = rows // 2
    w = 128
    nc = fq // w
    na = 4
    la = 8
    cw = 256
    npr = dq // cw
    tm = 512
    nz = ra // tm
    ne = tm + 64
    nn = ra - ne
    nl = 2 * npr - 1
    nk = nl + nz * (4 * npr - nl)
    no = nz * 2 * npr
    lag = 4
    oslots = 8
    xc = 2
    xrc = ra // xc
    own, oth = ra, 0

    def kernel(x, wg, wu, wd,
               z, wdy, wpo, wpx, ddy, dpo, dpx, d2o, d2p,
               xg, h, h2, wbuf, wlast, dbuf, zs, zr, zacc, zo, zoe,
               xs, xr, wys, wyr, wfs, wfr, hs, hr, bs, br,
               dys, dyr, dfs, dfr, d2s, d2r, d2t, d2u,
               zss, zsr, zos, zor, zls, lds):
        dz = lax.axis_index("dz")
        dy = lax.axis_index("dy")
        dx = lax.axis_index("dx")
        to_dz = {"dz": 1 - dz}
        to_dy = {"dy": 1 - dy}
        to_dx = {"dx": 1 - dx}

        def rcopy(src, dst, ss, rs, dev):
            return pltpu.make_async_remote_copy(
                src_ref=src, dst_ref=dst, send_sem=ss, recv_sem=rs, device_id=dev, device_id_type=MESH)

        mine = pl.multiple_of(dy * ra, ra)
        theirs = pl.multiple_of((1 - dy) * ra, ra)
        left, right = pl.ds(0, dh), pl.ds(dh, dh)

        def x_dy(i):
            return rcopy(x.at[pl.ds(theirs + i * xrc, xrc)], xg.at[pl.ds(own + i * xrc, xrc), right],
                         xs.at[i], xr.at[i], to_dy)

        def x_fw(i):
            return rcopy(xg.at[pl.ds(own + i * xrc, xrc), right], xg.at[pl.ds(oth + i * xrc, xrc), right],
                         xs.at[xc + i], xr.at[xc + i], to_dz)

        x_dz = rcopy(x.at[pl.ds(mine, ra)], xg.at[pl.ds(oth, ra), left], xs.at[2 * xc], xr.at[2 * xc], to_dz)
        x_lo = pltpu.make_async_copy(x.at[pl.ds(mine, ra)], xg.at[pl.ds(own, ra), left], lds.at[8])

        def cols(j):
            return pl.ds(pl.multiple_of(j * w, w), w)

        def w_dy(j):
            return [rcopy(src.at[:, cols(j)], wdy.at[j, t], wys.at[j, t], wyr.at[j, t], to_dy)
                    for t, src in enumerate((wg, wu))]

        def w_fw(j):
            return [rcopy(wdy.at[j, t], wpx.at[j, t], wfs.at[j, t], wfr.at[j, t], to_dx) for t in range(2)]

        lc, rc = pl.ds(0, w), pl.ds(w, w)
        jl = nc - 1
        w_dy_last = [rcopy(src.at[:, pl.ds(jl * w, w)], wlast.at[t, right, lc], wys.at[jl, t], wyr.at[jl, t], to_dy)
                     for t, src in enumerate((wg, wu))]
        w_fw_last = [rcopy(wlast.at[t, right, lc], wlast.at[t, right, rc], wfs.at[jl, t], wfr.at[jl, t], to_dx)
                     for t in range(2)]
        ld_last = [pltpu.make_async_copy(src.at[:, pl.ds(jl * w, w)], wlast.at[t, left, c], lds.at[9 + 2 * i + t])
                   for i, (srcs, c) in enumerate((((wg, wu), lc), ((wpo.at[0], wpo.at[1]), rc)))
                   for t, src in enumerate(srcs)]

        def dcols(p):
            return pl.ds(pl.multiple_of(p * cw, cw), cw)

        def d_dy(p):
            return rcopy(wd.at[:, dcols(p)], ddy.at[p], dys.at[p], dyr.at[p], to_dy)

        def d_fw(p):
            return rcopy(ddy.at[p], dpx.at[p], dfs.at[p], dfr.at[p], to_dx)

        bulk = [rcopy(src, dst, bs.at[i], br.at[i], to_dx)
                for i, (src, dst) in enumerate(((wg, wpo.at[0]), (wu, wpo.at[1]), (wd, dpo)))]

        def d2_dz(p):
            return rcopy(wd.at[:, dcols(p)], d2o.at[p], d2s.at[p], d2r.at[p], to_dz)

        def d2_fw(p):
            return rcopy(d2o.at[p], d2p.at[p], d2t.at[p], d2u.at[p], to_dx)

        def hcols(j, t):
            return pl.ds(pl.multiple_of(((dx + t) % 2) * fq + j * w, w), w)

        def h_dz(j, t):
            return rcopy(h.at[pl.ds(oth, ne), hcols(j, t)], h2.at[:, hcols(j, t)], hs.at[j, t], hr.at[j, t], to_dz)

        def start(cs):
            for c in cs:
                c.start()

        def wait_all(cs):
            for c in cs:
                c.wait()

        def wait_recv(cs):
            for c in cs:
                c.wait_recv()

        barrier = pltpu.get_barrier_semaphore()
        for dev in (to_dx, to_dy, to_dz):
            pl.semaphore_signal(barrier, inc=1, device_id=dev, device_id_type=MESH)
        pl.semaphore_wait(barrier, 3)

        for i in range(xc):
            x_dy(i).start()
        x_dz.start()
        x_lo.start()
        start(bulk[:2])

        @pl.loop(0, la)
        def _(j):
            start(w_dy(j))

        for i in range(xc):
            x_dy(i).wait_recv()
            x_fw(i).start()
        for p in range(npr - 1):
            d2_dz(p).start()

        @pl.when(dx == 0)
        def _():
            d2_dz(npr - 1).start()

        bulk[2].start()
        x_lo.wait()
        first_d = pltpu.make_async_copy(wd.at[:, dcols(0)], dbuf.at[0], lds.at[8])
        first_d.start()
        wait_recv(bulk[:2])

        def gate_up(row, n, j, wb):
            rs = pl.ds(pl.multiple_of(row, 64), n)
            xt = xg[rs, :]
            g = jnp.dot(xt, wb[0], preferred_element_type=F32).astype(BF16).astype(F32)
            u = jnp.dot(xt, wb[1], preferred_element_type=F32).astype(BF16).astype(F32)
            val = (g * jax.nn.sigmoid(g) * u).astype(BF16)
            for t in range(2):
                h[rs, hcols(j, t)] = val[:, t * w:(t + 1) * w]

        def rest(j, wb):
            gate_up(oth, ne, j, wb)

            @pl.loop(0, nz)
            def _(i):
                gate_up(own + i * tm, tm, j, wb)

                @pl.when(i == 0)
                def _():
                    h_dz(j, 0).start()
                    h_dz(j, 1).start()

        def loads(j):
            return [pltpu.make_async_copy(wg.at[:, cols(j)], wbuf.at[0, left, lc], lds.at[0]),
                    pltpu.make_async_copy(wu.at[:, cols(j)], wbuf.at[1, left, lc], lds.at[1]),
                    pltpu.make_async_copy(wpo.at[0, :, cols(j)], wbuf.at[0, left, rc], lds.at[2]),
                    pltpu.make_async_copy(wpo.at[1, :, cols(j)], wbuf.at[1, left, rc], lds.at[3]),
                    pltpu.make_async_copy(wdy.at[j, 0], wbuf.at[0, right, lc], lds.at[4]),
                    pltpu.make_async_copy(wdy.at[j, 1], wbuf.at[1, right, lc], lds.at[5]),
                    pltpu.make_async_copy(wpx.at[j, 0], wbuf.at[0, right, rc], lds.at[6]),
                    pltpu.make_async_copy(wpx.at[j, 1], wbuf.at[1, right, rc], lds.at[7])]

        def arrive(j):
            @pl.when(j + la < jl)
            def _():
                start(w_dy(j + la))

            @pl.when(j + la == jl)
            def _():
                start(w_dy_last)

            wait_recv(w_dy(j))
            start(w_fw(j))
            ld = loads(j)
            start(ld[:6])
            wait_recv(w_fw(j))
            start(ld[6:])
            wait_all(ld)

        @pl.loop(0, na)
        def _(j):
            arrive(j)

            @pl.loop(0, nz)
            def _(i):
                gate_up(own + i * tm, tm, j, wbuf)

        start(ld_last)
        x_dz.wait_recv()
        for i in range(xc):
            x_fw(i).wait_recv()

        @pl.loop(0, na)
        def _(j):
            ld = loads(j)
            start(ld)
            wait_all(ld)

            gate_up(oth, ne, j, wbuf)
            gate_up(oth + ne, nn, j, wbuf)
            h_dz(j, 0).start()
            h_dz(j, 1).start()

        @pl.loop(na, jl)
        def _(j):
            @pl.when(jnp.logical_and(j >= la, j < la + npr))
            def _():
                d_dy(j - la).start()

            @pl.when(jnp.logical_and(j >= nc - npr - 1, j < nc - 2))
            def _():
                p = j - (nc - npr - 1)
                d2_dz(p).wait_recv()
                d2_fw(p).start()

            @pl.when(jnp.logical_and(dx == 0, j == nc - 2))
            def _():
                d2_dz(npr - 1).wait_recv()
                d2_fw(npr - 1).start()

            arrive(j)
            gate_up(oth + ne, nn, j, wbuf)
            rest(j, wbuf)

        wait_all(ld_last)
        late_rows, late_part = pl.ds(oth + ne, nn), pl.ds(0, nn)
        for t in range(2):
            zs[1 + t, late_part] = jnp.dot(xg[late_rows, left], wlast[t, left], preferred_element_type=F32)
        first_d.wait()
        done = [(t * fq, fq - w) for t in range(2)]
        last = [(t * fq + fq - w, w) for t in range(2)]

        def z_sum(parts):
            return sum(jnp.dot(h[late_rows, pl.ds(a, n)], dbuf[0, pl.ds(a, n)], preferred_element_type=F32)
                       for a, n in parts)

        zacc[late_part] = z_sum(done)
        wait_recv(w_dy_last)
        start(w_fw_last)
        wait_recv(w_fw_last)
        xr_ = xg[late_rows, right]
        g, u = [(zs[1 + t, late_part] + jnp.dot(xr_, wlast[t, right], preferred_element_type=F32)).astype(BF16).astype(F32)
                for t in range(2)]
        val = (g * jax.nn.sigmoid(g) * u).astype(BF16)
        for t in range(2):
            h[late_rows, hcols(jl, t)] = val[:, t * w:(t + 1) * w]
        bulk[2].wait_recv()

        def split(k):
            late = (k + nk - nl) // nk
            s = (k - nl) // nz
            last = s // (2 * npr)
            odd = k // (nl - 1)
            half = late * (1 - last)
            p = (1 - late) * (k // 2) + late * ((1 - last) * (s // 2) + last * (npr - 1))
            q = (1 - late) * ((1 - odd) * (k % 2) + odd * dx) + late * ((1 - last) * (s % 2) + last * (1 - dx))
            r = (1 - late) * (nz - 1) + late * ((k - nl) % nz)
            return half, p, q, r

        def chunk_src(half, p, q):
            if half == 0:
                return (wd, dpo)[q].at[:, dcols(p)]
            return (ddy, dpx)[q].at[p]

        def load_d(k, slot, ok):
            half, p, q, r = split(k)
            ok = jnp.logical_and(ok, jnp.logical_or(k < nl, r == 0))
            for hh in range(2):
                for qq in range(2):
                    @pl.when(jnp.logical_and(ok, jnp.logical_and(half == hh, q == qq)))
                    def _(hh=hh, qq=qq):
                        c = pltpu.make_async_copy(chunk_src(hh, p, qq), dbuf.at[slot], lds.at[slot])
                        c.start()
                        c.wait()

        def sized(k, fn):
            _, _, _, r = split(k)

            @pl.when(k < nl)
            def _():
                fn(ne, nn)

            @pl.when(k >= nl)
            def _():
                fn(pl.multiple_of(r * tm, tm), tm)

        def z_send(k, n):
            return rcopy(zs.at[k % (lag + 1), pl.ds(0, n)], zr.at[k, pl.ds(0, n)], zss.at[k], zsr.at[k], to_dz)

        def out_cols(p, q):
            return pl.ds(pl.multiple_of(((dx + q) % 2) * dq + p * cw, cw), cw)

        def out_at(m, base):
            half, p, q, r = split(m)
            return z.at[pl.ds(pl.multiple_of(base + r * tm, tm), tm), out_cols(p, q)]

        def is_other(m):
            return split(m)[0] == 1

        def out_local(m, row, n):
            _, p, q, _ = split(m)
            return pltpu.make_async_copy(zo.at[m % oslots, pl.ds(0, n)],
                                         z.at[pl.ds(pl.multiple_of(mine + row, 64), n), out_cols(p, q)],
                                         zls.at[m % oslots])

        def out_remote(m):
            i = m - nl
            return rcopy(zo.at[m % oslots], out_at(m, mine), zos.at[i], zor.at[i], to_dy)

        def in_remote(m):
            i = m - nl
            return rcopy(zo.at[m % oslots], out_at(m, theirs), zos.at[i], zor.at[i], to_dy)

        def free_out(m):
            @pl.when(is_other(m))
            def _():
                out_remote(m).wait_send()

            @pl.when(jnp.logical_not(is_other(m)))
            def _():
                sized(m, lambda row, n: out_local(m, row, n).wait())

        def send_piece(k):
            half, p, q, r = split(k)

            @pl.when(jnp.logical_and(jnp.logical_and(half == 1, q == 1), r == 0))
            def _():
                d_fw(p).wait_recv()

            load_d(k, 0, True)

            @pl.when(k > lag)
            def _():
                sized(k - lag - 1, lambda row, n: z_send(k - lag - 1, n).wait_send())

            def piece(row, n):
                zs[k % (lag + 1), pl.ds(0, n)] = jnp.dot(h[pl.ds(pl.multiple_of(oth + row, 64), n), :], dbuf[0],
                                                         preferred_element_type=F32)
                z_send(k, n).start()

            sized(k, piece)

        def e_out(e):
            _, p, q, _ = split(e)
            return pltpu.make_async_copy(zoe, z.at[pl.ds(mine, ne), out_cols(p, q)], zls.at[oslots])

        def e_piece(e):
            _, p, q, _ = split(e)
            for qq in range(2):
                @pl.when(q == qq)
                def _(qq=qq):
                    c = [pltpu.make_async_copy(chunk_src(0, p, qq), dbuf.at[2], lds.at[2]),
                         pltpu.make_async_copy((d2o, d2p)[qq].at[p], dbuf.at[3], lds.at[3])]
                    start(c)
                    wait_all(c)

            acc = jnp.dot(h[pl.ds(own, ne), :], dbuf[2], preferred_element_type=F32)
            acc = acc + jnp.dot(h2[...], dbuf[3], preferred_element_type=F32)

            @pl.when(e >= 1)
            def _():
                e_out(e - 1).wait()

            zoe[...] = acc.astype(BF16)
            e_out(e).start()

        e0 = 7

        zs[0, late_part] = zacc[late_part] + z_sum(last)
        z_send(0, nn).start()

        @pl.loop(0, nk + lag)
        def _(k):
            @pl.when(jnp.logical_and(k > 0, k < nk))
            def _():
                send_piece(k)

            @pl.when(k == lag - 1)
            def _():
                rest(jl, wlast)

            f = k - (nl - 1)

            @pl.when(jnp.logical_and(f >= 0, jnp.logical_and(f < 2 * nz * npr, f % (2 * nz) == 0)))
            def _():
                d_dy(f // (2 * nz)).wait_recv()
                d_fw(f // (2 * nz)).start()

            @pl.when(k == e0 - 1)
            def _():
                for p in range(npr - 1):
                    d2_fw(p).wait_recv()

                @pl.when(dx == 1)
                def _():
                    d2_fw(npr - 1).wait_recv()

                @pl.loop(0, nc)
                def _(j):
                    for t in range(2):
                        h_dz(j, t).wait_recv()

            @pl.when(jnp.logical_and(k >= e0, jnp.logical_and(k < e0 + 2 * nl, (k - e0) % 2 == 0)))
            def _():
                e_piece((k - e0) // 2)

            @pl.when(k >= lag)
            def _():
                m = k - lag
                half, p, q, r = split(m)
                load_d(m, 1, k >= lag)
                @pl.when(m >= oslots)
                def _():
                    free_out(m - oslots)

                def piece(row, n):
                    zacc[pl.ds(0, n)] = jnp.dot(h[pl.ds(pl.multiple_of(own + row, 64), n), :], dbuf[1],
                                                preferred_element_type=F32)
                    z_send(m, n).wait_recv()
                    zo[m % oslots, pl.ds(0, n)] = (zacc[pl.ds(0, n)] + zr[m, pl.ds(0, n)]).astype(BF16)

                sized(m, piece)

                @pl.when(half == 0)
                def _():
                    sized(m, lambda row, n: out_local(m, row, n).start())

                @pl.when(half == 1)
                def _():
                    out_remote(m).start()

        @pl.loop(nk - oslots, nk)
        def _(m):
            free_out(m)

        e_out(nl - 1).wait()
        for k in range(nk - lag - 1, nk):
            z_send(k, tm).wait_send()
        for i in range(xc):
            x_dy(i).wait_send()
            x_fw(i).wait_send()
        x_dz.wait_send()

        for c in w_dy_last + w_fw_last + [h_dz(jl, 0), h_dz(jl, 1)]:
            c.wait_send()

        @pl.loop(0, jl)
        def _(j):
            for c in w_dy(j) + w_fw(j) + [h_dz(j, 0), h_dz(j, 1)]:
                c.wait_send()

        @pl.loop(0, npr)
        def _(p):
            d_dy(p).wait_send()
            d_fw(p).wait_send()

        for c in bulk:
            c.wait_send()
        for p in range(npr - 1):
            d2_dz(p).wait_send()
            d2_fw(p).wait_send()

        @pl.when(dx == 0)
        def _():
            d2_dz(npr - 1).wait_send()
            d2_fw(npr - 1).wait_send()

        @pl.loop(nl, nl + no)
        def _(m):
            in_remote(m).wait_recv()

    def sd(shape, dtype=BF16):
        return jax.ShapeDtypeStruct(shape, dtype)

    wl, dl = sd((nc, 2, dh, w)), sd((npr, fh, cw))
    outs = (sd((rows, dh)), wl, sd((2, dh, fq)), wl, dl, sd((fh, dq)), dl, dl, dl)
    dma = pltpu.SemaphoreType.DMA
    return pl.pallas_call(
        kernel,
        out_shape=outs,
        in_specs=[pl.BlockSpec(memory_space=pl.ANY)] * 4,
        out_specs=[pl.BlockSpec(memory_space=pl.ANY)] * len(outs),
        scratch_shapes=[
            pltpu.VMEM((rows, 2 * dh), BF16),
            pltpu.VMEM((rows, fh), BF16),
            pltpu.VMEM((ne, fh), BF16),
            pltpu.VMEM((2, 2 * dh, 2 * w), BF16),
            pltpu.VMEM((2, 2 * dh, 2 * w), BF16),
            pltpu.VMEM((4, fh, cw), BF16),
            pltpu.VMEM((lag + 1, tm, cw), F32),
            pltpu.VMEM((nk, tm, cw), F32),
            pltpu.VMEM((tm, cw), F32),
            pltpu.VMEM((oslots, tm, cw), BF16),
            pltpu.VMEM((ne, cw), BF16),
            dma((2 * xc + 1,)), dma((2 * xc + 1,)),
            dma((nc, 2)), dma((nc, 2)), dma((nc, 2)), dma((nc, 2)), dma((nc, 2)), dma((nc, 2)), dma((3,)), dma((3,)),
            dma((npr,)), dma((npr,)), dma((npr,)), dma((npr,)), dma((npr,)), dma((npr,)), dma((npr,)), dma((npr,)),
            dma((nk,)), dma((nk,)), dma((no,)), dma((no,)), dma((oslots + 1,)), dma((13,)),
        ],
        compiler_params=pltpu.CompilerParams(
            collective_id=0, has_side_effects=True, vmem_limit_bytes=67043328),
    )


def copy_rows(shape):
    n = 8
    rows = shape[0] // n

    def kernel(src, dst, buf, rs, ws):
        part = [pl.ds(i * rows, rows) for i in range(n)]
        reads = [pltpu.make_async_copy(src.at[p], buf.at[p], rs.at[i]) for i, p in enumerate(part)]
        writes = [pltpu.make_async_copy(buf.at[p], dst.at[p], ws.at[i]) for i, p in enumerate(part)]
        for r in reads:
            r.start()
        for r, c in zip(reads, writes):
            r.wait()
            c.start()
        for c in writes:
            c.wait()

    return pl.pallas_call(
        kernel,
        out_shape=jax.ShapeDtypeStruct(shape, BF16),
        in_specs=[pl.BlockSpec(memory_space=pl.ANY)],
        out_specs=pl.BlockSpec(memory_space=pl.ANY),
        scratch_shapes=[pltpu.VMEM(shape, BF16), pltpu.SemaphoreType.DMA((n,)), pltpu.SemaphoreType.DMA((n,))],
    )


def solution(mesh):
    x_spec = P(("grp", "dx", "dz"), "dy")
    w_in_spec = P("dy", ("dz", "dx"))
    w_out_spec = P("dz", ("dy", "dx"))

    def local_mlp(x_blk, wg_blk, wu_blk, wd_blk):
        outs = make_local_mlp(x_blk.shape, wg_blk.shape, wd_blk.shape)(x_blk, wg_blk, wu_blk, wd_blk)
        return copy_rows(x_blk.shape)(outs[0])

    return jax.shard_map(local_mlp, mesh=mesh, in_specs=(x_spec, w_in_spec, w_in_spec, w_out_spec), out_specs=x_spec, check_vma=False)
```

```python
import jax
import jax.numpy as jnp
from jax import lax
from jax.experimental import pallas as pl
from jax.experimental.pallas import tpu as pltpu
from jax.sharding import PartitionSpec as P

MESH = pl.DeviceIdType.MESH
BF16 = jnp.bfloat16
F32 = jnp.float32


def make_local_mlp(x_shape, w_shape, d_shape):
    rows, dh = x_shape
    fq = w_shape[1]
    fh, dq = d_shape
    ra = rows // 2
    w = 128
    nc = fq // w
    na = 4
    la = 8
    cw = 256
    npr = dq // cw
    tm = 512
    nz = ra // tm
    ne = tm + 64
    nn = ra - ne
    nl = 2 * npr - 1
    nk = nl + nz * (4 * npr - nl)
    no = nz * 2 * npr
    lag = 2
    oslots = 5
    xc = 2
    xrc = ra // xc
    own, oth = ra, 0

    def kernel(x, wg, wu, wd,
               z, wdy, wpo, wpx, ddy, dpo, dpx, d2o, d2p,
               xg, h, h2, wbuf, wlast, dbuf, zs, zr, zacc, zo,
               xs, xr, wys, wyr, wfs, wfr, hs, hr, bs, br,
               dys, dyr, dfs, dfr, d2s, d2r, d2t, d2u,
               zss, zsr, zos, zor, lds):
        dz = lax.axis_index("dz")
        dy = lax.axis_index("dy")
        dx = lax.axis_index("dx")
        to_dz = {"dz": 1 - dz}
        to_dy = {"dy": 1 - dy}
        to_dx = {"dx": 1 - dx}

        def rcopy(src, dst, ss, rs, dev):
            return pltpu.make_async_remote_copy(
                src_ref=src, dst_ref=dst, send_sem=ss, recv_sem=rs, device_id=dev, device_id_type=MESH)

        mine = pl.multiple_of(dy * ra, ra)
        theirs = pl.multiple_of((1 - dy) * ra, ra)
        left, right = pl.ds(0, dh), pl.ds(dh, dh)

        def x_dy(i):
            return rcopy(x.at[pl.ds(theirs + i * xrc, xrc)], xg.at[pl.ds(own + i * xrc, xrc), right],
                         xs.at[i], xr.at[i], to_dy)

        def x_fw(i):
            return rcopy(xg.at[pl.ds(own + i * xrc, xrc), right], xg.at[pl.ds(oth + i * xrc, xrc), right],
                         xs.at[xc + i], xr.at[xc + i], to_dz)

        x_dz = rcopy(x.at[pl.ds(mine, ra)], xg.at[pl.ds(oth, ra), left], xs.at[2 * xc], xr.at[2 * xc], to_dz)
        x_lo = pltpu.make_async_copy(x.at[pl.ds(mine, ra)], xg.at[pl.ds(own, ra), left], lds.at[8])

        def cols(j):
            return pl.ds(pl.multiple_of(j * w, w), w)

        def w_dy(j):
            return [rcopy(src.at[:, cols(j)], wdy.at[j, t], wys.at[j, t], wyr.at[j, t], to_dy)
                    for t, src in enumerate((wg, wu))]

        def w_fw(j):
            return [rcopy(wdy.at[j, t], wpx.at[j, t], wfs.at[j, t], wfr.at[j, t], to_dx) for t in range(2)]

        lc, rc = pl.ds(0, w), pl.ds(w, w)
        jl = nc - 1
        w_dy_last = [rcopy(src.at[:, pl.ds(jl * w, w)], wlast.at[t, right, lc], wys.at[jl, t], wyr.at[jl, t], to_dy)
                     for t, src in enumerate((wg, wu))]
        w_fw_last = [rcopy(wlast.at[t, right, lc], wlast.at[t, right, rc], wfs.at[jl, t], wfr.at[jl, t], to_dx)
                     for t in range(2)]
        ld_last = [pltpu.make_async_copy(src.at[:, pl.ds(jl * w, w)], wlast.at[t, left, c], lds.at[9 + 2 * i + t])
                   for i, (srcs, c) in enumerate((((wg, wu), lc), ((wpo.at[0], wpo.at[1]), rc)))
                   for t, src in enumerate(srcs)]

        def dcols(p):
            return pl.ds(pl.multiple_of(p * cw, cw), cw)

        def d_dy(p):
            return rcopy(wd.at[:, dcols(p)], ddy.at[p], dys.at[p], dyr.at[p], to_dy)

        def d_fw(p):
            return rcopy(ddy.at[p], dpx.at[p], dfs.at[p], dfr.at[p], to_dx)

        bulk = [rcopy(src, dst, bs.at[i], br.at[i], to_dx)
                for i, (src, dst) in enumerate(((wg, wpo.at[0]), (wu, wpo.at[1]), (wd, dpo)))]

        def d2_dz(p):
            return rcopy(wd.at[:, dcols(p)], d2o.at[p], d2s.at[p], d2r.at[p], to_dz)

        def d2_fw(p):
            return rcopy(d2o.at[p], d2p.at[p], d2t.at[p], d2u.at[p], to_dx)

        def hcols(j, t):
            return pl.ds(pl.multiple_of(((dx + t) % 2) * fq + j * w, w), w)

        def h_dz(j, t):
            return rcopy(h.at[pl.ds(oth, ne), hcols(j, t)], h2.at[:, hcols(j, t)], hs.at[j, t], hr.at[j, t], to_dz)

        def start(cs):
            for c in cs:
                c.start()

        def wait_all(cs):
            for c in cs:
                c.wait()

        def wait_recv(cs):
            for c in cs:
                c.wait_recv()

        barrier = pltpu.get_barrier_semaphore()
        for dev in (to_dx, to_dy, to_dz):
            pl.semaphore_signal(barrier, inc=1, device_id=dev, device_id_type=MESH)
        pl.semaphore_wait(barrier, 3)

        for i in range(xc):
            x_dy(i).start()
        x_dz.start()
        x_lo.start()
        start(bulk[:2])

        @pl.loop(0, la)
        def _(j):
            start(w_dy(j))

        for i in range(xc):
            x_dy(i).wait_recv()
            x_fw(i).start()
        for p in range(npr - 1):
            d2_dz(p).start()

        @pl.when(dx == 0)
        def _():
            d2_dz(npr - 1).start()

        bulk[2].start()
        x_lo.wait()
        first_d = pltpu.make_async_copy(wd.at[:, dcols(0)], dbuf.at[0], lds.at[8])
        first_d.start()
        wait_recv(bulk[:2])

        def gate_up(row, n, j, wb):
            rs = pl.ds(pl.multiple_of(row, 64), n)
            xt = xg[rs, :]
            g = jnp.dot(xt, wb[0], preferred_element_type=F32).astype(BF16).astype(F32)
            u = jnp.dot(xt, wb[1], preferred_element_type=F32).astype(BF16).astype(F32)
            val = (g * jax.nn.sigmoid(g) * u).astype(BF16)
            for t in range(2):
                h[rs, hcols(j, t)] = val[:, t * w:(t + 1) * w]

        def rest(j, wb):
            gate_up(oth, ne, j, wb)

            @pl.loop(0, nz)
            def _(i):
                gate_up(own + i * tm, tm, j, wb)

                @pl.when(i == 0)
                def _():
                    h_dz(j, 0).start()
                    h_dz(j, 1).start()

        def loads(j):
            return [pltpu.make_async_copy(wg.at[:, cols(j)], wbuf.at[0, left, lc], lds.at[0]),
                    pltpu.make_async_copy(wu.at[:, cols(j)], wbuf.at[1, left, lc], lds.at[1]),
                    pltpu.make_async_copy(wpo.at[0, :, cols(j)], wbuf.at[0, left, rc], lds.at[2]),
                    pltpu.make_async_copy(wpo.at[1, :, cols(j)], wbuf.at[1, left, rc], lds.at[3]),
                    pltpu.make_async_copy(wdy.at[j, 0], wbuf.at[0, right, lc], lds.at[4]),
                    pltpu.make_async_copy(wdy.at[j, 1], wbuf.at[1, right, lc], lds.at[5]),
                    pltpu.make_async_copy(wpx.at[j, 0], wbuf.at[0, right, rc], lds.at[6]),
                    pltpu.make_async_copy(wpx.at[j, 1], wbuf.at[1, right, rc], lds.at[7])]

        def arrive(j):
            @pl.when(j + la < jl)
            def _():
                start(w_dy(j + la))

            @pl.when(j + la == jl)
            def _():
                start(w_dy_last)

            wait_recv(w_dy(j))
            start(w_fw(j))
            ld = loads(j)
            start(ld[:6])
            wait_recv(w_fw(j))
            start(ld[6:])
            wait_all(ld)

        @pl.loop(0, na)
        def _(j):
            arrive(j)

            @pl.loop(0, nz)
            def _(i):
                gate_up(own + i * tm, tm, j, wbuf)

        start(ld_last)
        x_dz.wait_recv()
        for i in range(xc):
            x_fw(i).wait_recv()

        @pl.loop(0, na)
        def _(j):
            ld = loads(j)
            start(ld)
            wait_all(ld)

            gate_up(oth, ne, j, wbuf)
            gate_up(oth + ne, nn, j, wbuf)
            h_dz(j, 0).start()
            h_dz(j, 1).start()

        @pl.loop(na, jl)
        def _(j):
            @pl.when(jnp.logical_and(j >= la, j < la + npr))
            def _():
                d_dy(j - la).start()

            @pl.when(jnp.logical_and(j >= nc - npr - 1, j < nc - 2))
            def _():
                p = j - (nc - npr - 1)
                d2_dz(p).wait_recv()
                d2_fw(p).start()

            @pl.when(jnp.logical_and(dx == 0, j == nc - 2))
            def _():
                d2_dz(npr - 1).wait_recv()
                d2_fw(npr - 1).start()

            arrive(j)
            gate_up(oth + ne, nn, j, wbuf)
            rest(j, wbuf)

        wait_all(ld_last)
        late_rows, late_part = pl.ds(oth + ne, nn), pl.ds(0, nn)
        for t in range(2):
            zs[1 + t, late_part] = jnp.dot(xg[late_rows, left], wlast[t, left], preferred_element_type=F32)
        first_d.wait()
        done = [(t * fq, fq - w) for t in range(2)]
        last = [(t * fq + fq - w, w) for t in range(2)]

        def z_sum(parts):
            return sum(jnp.dot(h[late_rows, pl.ds(a, n)], dbuf[0, pl.ds(a, n)], preferred_element_type=F32)
                       for a, n in parts)

        zacc[late_part] = z_sum(done)
        wait_recv(w_dy_last)
        start(w_fw_last)
        wait_recv(w_fw_last)
        xr_ = xg[late_rows, right]
        g, u = [(zs[1 + t, late_part] + jnp.dot(xr_, wlast[t, right], preferred_element_type=F32)).astype(BF16).astype(F32)
                for t in range(2)]
        val = (g * jax.nn.sigmoid(g) * u).astype(BF16)
        for t in range(2):
            h[late_rows, hcols(jl, t)] = val[:, t * w:(t + 1) * w]
        bulk[2].wait_recv()

        def split(k):
            late = (k + nk - nl) // nk
            s = (k - nl) // nz
            last = s // (2 * npr)
            odd = k // (nl - 1)
            half = late * (1 - last)
            p = (1 - late) * (k // 2) + late * ((1 - last) * (s // 2) + last * (npr - 1))
            q = (1 - late) * ((1 - odd) * (k % 2) + odd * dx) + late * ((1 - last) * (s % 2) + last * (1 - dx))
            r = (1 - late) * (nz - 1) + late * ((k - nl) % nz)
            return half, p, q, r

        def chunk_src(half, p, q):
            if half == 0:
                return (wd, dpo)[q].at[:, dcols(p)]
            return (ddy, dpx)[q].at[p]

        def load_d(k, slot, ok):
            half, p, q, r = split(k)
            ok = jnp.logical_and(ok, jnp.logical_or(k < nl, r == 0))
            for hh in range(2):
                for qq in range(2):
                    @pl.when(jnp.logical_and(ok, jnp.logical_and(half == hh, q == qq)))
                    def _(hh=hh, qq=qq):
                        c = pltpu.make_async_copy(chunk_src(hh, p, qq), dbuf.at[slot], lds.at[slot])
                        c.start()
                        c.wait()

        def sized(k, fn):
            _, _, _, r = split(k)

            @pl.when(k < nl)
            def _():
                fn(ne, nn)

            @pl.when(k >= nl)
            def _():
                fn(pl.multiple_of(r * tm, tm), tm)

        def z_send(k, n):
            return rcopy(zs.at[k % (lag + 1), pl.ds(0, n)], zr.at[k, pl.ds(0, n)], zss.at[k], zsr.at[k], to_dz)

        def out_cols(p, q):
            return pl.ds(pl.multiple_of(((dx + q) % 2) * dq + p * cw, cw), cw)

        def out_at(m, base):
            _, p, q, r = split(m)
            return z.at[pl.ds(pl.multiple_of(base + r * tm, tm), tm), out_cols(p, q)]

        def out_remote(i):
            return rcopy(zo.at[i % oslots], out_at(i + nl, mine), zos.at[i], zor.at[i], to_dy)

        def in_remote(i):
            return rcopy(zo.at[i % oslots], out_at(i + nl, theirs), zos.at[i], zor.at[i], to_dy)

        def send_piece(k):
            half, p, q, r = split(k)

            @pl.when(jnp.logical_and(jnp.logical_and(half == 1, q == 1), r == 0))
            def _():
                d_fw(p).wait_recv()

            load_d(k, 0, True)

            @pl.when(k > lag)
            def _():
                sized(k - lag - 1, lambda row, n: z_send(k - lag - 1, n).wait_send())

            def piece(row, n):
                zs[k % (lag + 1), pl.ds(0, n)] = jnp.dot(h[pl.ds(pl.multiple_of(oth + row, 64), n), :], dbuf[0],
                                                         preferred_element_type=F32)
                z_send(k, n).start()

            sized(k, piece)

        parts = [(i, 2 * dh * i, min(2 * dh, fh - 2 * dh * i)) for i in range(2)]

        def e_piece(e):
            _, p, q, _ = split(e)
            for qq in range(2):
                @pl.when(q == qq)
                def _(qq=qq):
                    c = [pltpu.make_async_copy(src.at[pl.ds(a, n)], buf.at[i, pl.ds(0, n)], lds.at[2 + 2 * b + i])
                         for b, (src, buf) in enumerate(((chunk_src(0, p, qq), wbuf), ((d2o, d2p)[qq].at[p], wlast)))
                         for i, a, n in parts]
                    start(c)
                    wait_all(c)

            acc = sum(jnp.dot(lhs[pl.ds(r0, ne), pl.ds(a, n)], buf[i, pl.ds(0, n)], preferred_element_type=F32)
                      for lhs, r0, buf in ((h, own, wbuf), (h2, 0, wlast)) for i, a, n in parts)
            z[pl.ds(mine, ne), out_cols(p, q)] = acc.astype(BF16)

        e0 = 7

        zs[0, late_part] = zacc[late_part] + z_sum(last)
        z_send(0, nn).start()

        @pl.loop(0, nk + lag)
        def _(k):
            @pl.when(jnp.logical_and(k > 0, k < nk))
            def _():
                send_piece(k)

            @pl.when(k == lag - 1)
            def _():
                rest(jl, wlast)

            f = k - (nl - 1)

            @pl.when(jnp.logical_and(f >= 0, jnp.logical_and(f < 2 * nz * npr, f % (2 * nz) == 0)))
            def _():
                d_dy(f // (2 * nz)).wait_recv()
                d_fw(f // (2 * nz)).start()

            @pl.when(k == e0 - 1)
            def _():
                for c in w_fw_last:
                    c.wait_send()

                for p in range(npr - 1):
                    d2_fw(p).wait_recv()

                @pl.when(dx == 1)
                def _():
                    d2_fw(npr - 1).wait_recv()

                @pl.loop(0, nc)
                def _(j):
                    for t in range(2):
                        h_dz(j, t).wait_recv()

            @pl.when(jnp.logical_and(k >= e0, jnp.logical_and(k < e0 + 2 * nl, (k - e0) % 2 == 0)))
            def _():
                e_piece((k - e0) // 2)

            @pl.when(k >= lag)
            def _():
                m = k - lag
                half, p, q, r = split(m)
                load_d(m, 1, k >= lag)
                i = m - nl

                @pl.when(jnp.logical_and(i >= oslots, i < no))
                def _():
                    out_remote(i - oslots).wait_send()

                def piece(row, n):
                    zacc[pl.ds(0, n)] = jnp.dot(h[pl.ds(pl.multiple_of(own + row, 64), n), :], dbuf[1],
                                                preferred_element_type=F32)
                    z_send(m, n).wait_recv()
                    val = (zacc[pl.ds(0, n)] + zr[m, pl.ds(0, n)]).astype(BF16)

                    @pl.when(half == 0)
                    def _():
                        z[pl.ds(pl.multiple_of(mine + row, 64), n), out_cols(p, q)] = val

                    @pl.when(half == 1)
                    def _():
                        zo[jnp.maximum(i, 0) % oslots, pl.ds(0, n)] = val

                sized(m, piece)

                @pl.when(half == 1)
                def _():
                    out_remote(i).start()

        @pl.loop(no - oslots, no)
        def _(i):
            out_remote(i).wait_send()

        for k in range(nk - lag - 1, nk):
            z_send(k, tm).wait_send()
        for i in range(xc):
            x_dy(i).wait_send()
            x_fw(i).wait_send()
        x_dz.wait_send()

        for c in w_dy_last + [h_dz(jl, 0), h_dz(jl, 1)]:
            c.wait_send()

        @pl.loop(0, jl)
        def _(j):
            for c in w_dy(j) + w_fw(j) + [h_dz(j, 0), h_dz(j, 1)]:
                c.wait_send()

        @pl.loop(0, npr)
        def _(p):
            d_dy(p).wait_send()
            d_fw(p).wait_send()

        for c in bulk:
            c.wait_send()
        for p in range(npr - 1):
            d2_dz(p).wait_send()
            d2_fw(p).wait_send()

        @pl.when(dx == 0)
        def _():
            d2_dz(npr - 1).wait_send()
            d2_fw(npr - 1).wait_send()

        @pl.loop(0, no)
        def _(i):
            in_remote(i).wait_recv()

    def sd(shape, dtype=BF16):
        return jax.ShapeDtypeStruct(shape, dtype)

    wl, dl = sd((nc, 2, dh, w)), sd((npr, fh, cw))
    outs = (pltpu.VMEM((rows, dh), BF16), wl, sd((2, dh, fq)), wl, dl, sd((fh, dq)), dl, dl, dl)
    dma = pltpu.SemaphoreType.DMA
    return pl.pallas_call(
        kernel,
        out_shape=outs,
        in_specs=[pl.BlockSpec(memory_space=pl.ANY)] * 4,
        out_specs=[pl.BlockSpec(memory_space=pltpu.VMEM)] + [pl.BlockSpec(memory_space=pl.ANY)] * (len(outs) - 1),
        scratch_shapes=[
            pltpu.VMEM((rows, 2 * dh), BF16),
            pltpu.VMEM((rows, fh), BF16),
            pltpu.VMEM((ne, fh), BF16),
            pltpu.VMEM((2, 2 * dh, 2 * w), BF16),
            pltpu.VMEM((2, 2 * dh, 2 * w), BF16),
            pltpu.VMEM((2, fh, cw), BF16),
            pltpu.VMEM((lag + 1, tm, cw), F32),
            pltpu.VMEM((nk, tm, cw), F32),
            pltpu.VMEM((tm, cw), F32),
            pltpu.VMEM((oslots, tm, cw), BF16),
            dma((2 * xc + 1,)), dma((2 * xc + 1,)),
            dma((nc, 2)), dma((nc, 2)), dma((nc, 2)), dma((nc, 2)), dma((nc, 2)), dma((nc, 2)), dma((3,)), dma((3,)),
            dma((npr,)), dma((npr,)), dma((npr,)), dma((npr,)), dma((npr,)), dma((npr,)), dma((npr,)), dma((npr,)),
            dma((nk,)), dma((nk,)), dma((no,)), dma((no,)), dma((13,)),
        ],
        compiler_params=pltpu.CompilerParams(
            collective_id=0, has_side_effects=True, vmem_limit_bytes=67043328 - 2 * rows * dh),
    )


def solution(mesh):
    x_spec = P(("grp", "dx", "dz"), "dy")
    w_in_spec = P("dy", ("dz", "dx"))
    w_out_spec = P("dz", ("dy", "dx"))

    def local_mlp(x_blk, wg_blk, wu_blk, wd_blk):
        return make_local_mlp(x_blk.shape, wg_blk.shape, wd_blk.shape)(x_blk, wg_blk, wu_blk, wd_blk)[0]

    return jax.shard_map(local_mlp, mesh=mesh, in_specs=(x_spec, w_in_spec, w_in_spec, w_out_spec), out_specs=x_spec, check_vma=False)
```
